16 devices in a mesh: fsdp: 2 (over z), model: 8 (over y, x, core).
Axes of the slice: x: 2, y: 2, z: 2, core: 2. Of those that a mesh axis runs over, the one named last changes fastest.
Arguments:
- x_in: bfloat16 [16, 256, 5120], P('fsdp', 'model')
- gain_attn: float32 [2, 5120], replicated
- gain_mlp: float32 [2, 5120], replicated
- rope_cos: float32 [256, 64], replicated
- rope_sin: float32 [256, 64], replicated
- w_q: bfloat16 [2, 5120, 5120], P(None, 'fsdp', 'model')
- w_k: bfloat16 [2, 5120, 1024], P(None, 'fsdp', 'model')
- w_v: bfloat16 [2, 5120, 1024], P(None, 'fsdp', 'model')
- w_o: bfloat16 [2, 5120, 5120], P(None, 'model', 'fsdp')
- w_gate: bfloat16 [2, 5120, 13824], P(None, 'fsdp', 'model')
- w_up: bfloat16 [2, 5120, 13824], P(None, 'fsdp', 'model')
- w_down: bfloat16 [2, 13824, 5120], P(None, 'model', 'fsdp')
Outputs:
- output: bfloat16 [16, 256, 5120], P('fsdp', 'model')
All inputs are finite; a program needn't handle non-finite values.
Results may differ from the reference program's by a relative error of at most 0.02.
Values are sent between devices in bfloat16 or wider.
A program may use at most 1 GiB of HBM per device.

```python
import math
import jax
import jax.numpy as jnp
from jax import lax

D_MODEL = 5120
FFN = 13824
HEADS = 40
KV_HEADS = 8
HEAD_DIM = 128
BATCH = 16
SEQ = 256
LAYERS = 2
EPS = 1e-5
ROPE_BASE = 500000.0


def rope_tables(rng_key):
    pos_steps = jax.random.randint(rng_key, (SEQ,), 1, 4)
    positions = (jnp.cumsum(pos_steps) - pos_steps[0]).astype(jnp.float32)
    inv_freq = ROPE_BASE ** (-jnp.arange(HEAD_DIM // 2, dtype=jnp.float32) * (2.0 / HEAD_DIM))
    angles = positions[:, None] * inv_freq[None, :]
    return jnp.cos(angles), jnp.sin(angles)


def setup_inputs(seed: int = 0) -> dict:
    key_list = jax.random.split(jax.random.key(seed), 12)
    q_scale = math.sqrt(max(1.0, math.log(SEQ / 16.0)))

    def normal(rng_key, arr_shape, std_scale):
        return (jax.random.normal(rng_key, arr_shape, jnp.float32) * std_scale).astype(jnp.bfloat16)

    rope_cos, rope_sin = rope_tables(key_list[3])
    return {
        'x_in': normal(key_list[0], (BATCH, SEQ, D_MODEL), 1.0),
        'gain_attn': jax.random.uniform(key_list[1], (LAYERS, D_MODEL), jnp.float32, 0.5, 1.5),
        'gain_mlp': jax.random.uniform(key_list[2], (LAYERS, D_MODEL), jnp.float32, 0.5, 1.5),
        'rope_cos': rope_cos,
        'rope_sin': rope_sin,
        'w_q': normal(key_list[4], (LAYERS, D_MODEL, HEADS * HEAD_DIM), q_scale * D_MODEL ** -0.5),
        'w_k': normal(key_list[5], (LAYERS, D_MODEL, KV_HEADS * HEAD_DIM), D_MODEL ** -0.5),
        'w_v': normal(key_list[6], (LAYERS, D_MODEL, KV_HEADS * HEAD_DIM), D_MODEL ** -0.5),
        'w_o': normal(key_list[7], (LAYERS, HEADS * HEAD_DIM, D_MODEL), 2.0 * (HEADS * HEAD_DIM) ** -0.5),
        'w_gate': normal(key_list[8], (LAYERS, D_MODEL, FFN), D_MODEL ** -0.5),
        'w_up': normal(key_list[9], (LAYERS, D_MODEL, FFN), D_MODEL ** -0.5),
        'w_down': normal(key_list[10], (LAYERS, FFN, D_MODEL), FFN ** -0.5),
    }


def rms_norm(seq_rows, gain_vec):
    rows_f = seq_rows.astype(jnp.float32)
    mean_sq = jnp.mean(rows_f * rows_f, axis=-1, keepdims=True)
    return (rows_f * lax.rsqrt(mean_sq + EPS) * gain_vec).astype(jnp.bfloat16)


def rotate(head_vals, cos_b, sin_b):
    half_dim = head_vals.shape[-1] // 2
    heads_f = head_vals.astype(jnp.float32)
    first_half = heads_f[..., :half_dim]
    second_half = heads_f[..., half_dim:]
    return jnp.concatenate([first_half * cos_b - second_half * sin_b, second_half * cos_b + first_half * sin_b], axis=-1).astype(jnp.bfloat16)


def decoder_layer(seq_rows, params, rope_cos, rope_sin):
    gain_attn, gain_mlp, w_q, w_k, w_v, w_o, w_gate, w_up, w_down = params
    group_size = HEADS // KV_HEADS
    normed = rms_norm(seq_rows, gain_attn)
    q_proj = jnp.dot(normed, w_q, preferred_element_type=jnp.float32).astype(jnp.bfloat16).reshape(SEQ, KV_HEADS, group_size, HEAD_DIM)
    k_proj = jnp.dot(normed, w_k, preferred_element_type=jnp.float32).astype(jnp.bfloat16).reshape(SEQ, KV_HEADS, HEAD_DIM)
    v_proj = jnp.dot(normed, w_v, preferred_element_type=jnp.float32).astype(jnp.bfloat16).reshape(SEQ, KV_HEADS, HEAD_DIM)
    q_rot = rotate(q_proj, rope_cos[:, None, None, :], rope_sin[:, None, None, :])
    k_rot = rotate(k_proj, rope_cos[:, None, :], rope_sin[:, None, :])
    scores = jnp.einsum('qkgd,skd->kgqs', q_rot.astype(jnp.float32), k_rot.astype(jnp.float32)) * HEAD_DIM ** -0.5
    positions = jnp.arange(SEQ)
    causal = positions[:, None] >= positions[None, :]
    scores = jnp.where(causal, scores, -jnp.inf)
    attn_probs = jax.nn.softmax(scores, axis=-1).astype(jnp.bfloat16)
    attn_out = jnp.einsum('kgqs,skd->qkgd', attn_probs.astype(jnp.float32), v_proj.astype(jnp.float32)).astype(jnp.bfloat16).reshape(SEQ, HEADS * HEAD_DIM)
    attn_sum = jnp.dot(attn_out, w_o, preferred_element_type=jnp.float32)
    mid_rows = (seq_rows.astype(jnp.float32) + attn_sum).astype(jnp.bfloat16)
    normed_mlp = rms_norm(mid_rows, gain_mlp)
    gate_acc = jnp.dot(normed_mlp, w_gate, preferred_element_type=jnp.float32)
    up_acc = jnp.dot(normed_mlp, w_up, preferred_element_type=jnp.float32)
    hidden = (jax.nn.silu(gate_acc) * up_acc).astype(jnp.bfloat16)
    mlp_sum = jnp.dot(hidden, w_down, preferred_element_type=jnp.float32)
    return (mid_rows.astype(jnp.float32) + mlp_sum).astype(jnp.bfloat16)


def reference(x_in, gain_attn, gain_mlp, rope_cos, rope_sin, w_q, w_k, w_v, w_o, w_gate, w_up, w_down):
    params = (gain_attn, gain_mlp, w_q, w_k, w_v, w_o, w_gate, w_up, w_down)

    def one_sequence(seq_rows):
        def layer_step(carry_rows, layer_params):
            return decoder_layer(carry_rows, layer_params, rope_cos, rope_sin), None
        final_rows, _ = lax.scan(layer_step, seq_rows, params)
        return final_rows

    return lax.map(one_sequence, x_in)
```

```python
import functools

import jax
import jax.numpy as jnp
from jax import lax
from jax.experimental import pallas as pl
from jax.experimental.pallas import tpu as pltpu
from jax.sharding import PartitionSpec as P

EPS = 1e-5
MESH = pl.DeviceIdType.MESH
NT = (((1,), (1,)), ((), ()))
LD = 1
LX = 2
LT = LD + 2 * LX
LH = 2
F32 = jnp.float32
BF16 = jnp.bfloat16


def _norm(rows, gain):
    rows = rows.astype(F32)
    mean_sq = jnp.mean(rows * rows, axis=-1, keepdims=True)
    return (rows * lax.rsqrt(mean_sq + EPS) * gain).astype(BF16)


def _kernel(
    x_ref, ga_ref, gm_ref, cos_ref, sin_ref, wq_ref, wk_ref, wv_ref, wo_ref, wg_ref, wu_ref, wd_ref,
    y_ref, rq, rk, rv, ro, rg, ru, ha, hb,
    xbuf, mpeer, hst, hv, pown, psib, rd, t1, t2, rx, ry, rx2, ry2, hown, hrecv, cbuf, sbuf,
    zs, zr, gs, gr, ds, dr, xs, xr, ys, yr, x2s, x2r, y2s, y2r, ms, mr, os_, or_, hs, hr,
    sa, ra, sb, rb, loc, hvs, wl,
):
    n_layers = wq_ref.shape[0]
    NB, T, D = x_ref.shape
    W, V = D // 2, D // 4
    QW = wq_ref.shape[2]
    HD = wk_ref.shape[2]
    HB = wg_ref.shape[1] // 2
    R = 8 * T
    NU = 2 * NB

    z = lax.axis_index("fsdp")
    m = lax.axis_index("model")
    y, x, c, q = m // 4, (m // 2) % 2, m % 2, m // 2
    qx, qy, qd = q + 1 - 2 * x, q + 2 - 4 * y, 3 - q
    zp, xp, yp, sp = (1 - z, m), (z, m + 2 - 4 * x), (z, m + 4 - 8 * y), (z, m + 1 - 2 * c)
    mine = pl.ds(pl.multiple_of(z * W, 128), W)
    other = pl.ds(pl.multiple_of((1 - z) * W, 128), W)

    barrier = pltpu.get_barrier_semaphore()
    for dev in (zp, xp, yp, sp):
        pl.semaphore_signal(barrier, inc=1, device_id=dev, device_id_type=MESH)
    pl.semaphore_wait(barrier, 4)

    def send(src, dst, s, r, dev):
        return pltpu.make_async_remote_copy(
            src_ref=src, dst_ref=dst, send_sem=s, recv_sem=r, device_id=dev, device_id_type=MESH)

    def z_q(l):
        return send(wq_ref.at[l], rq.at[l], zs.at[0], zr.at[0], zp)

    def z_k(l):
        return send(wk_ref.at[l], rk.at[l], zs.at[1], zr.at[1], zp)

    def z_v(l):
        return send(wv_ref.at[l], rv.at[l], zs.at[2], zr.at[2], zp)

    def z_o(l):
        return send(wo_ref.at[l], ro.at[l], zs.at[3], zr.at[3], zp)

    theirs_h = pl.ds(pl.multiple_of((1 - z) * HB, 16), HB)

    def z_g(l):
        return send(wg_ref.at[l, theirs_h], rg.at[l], gs.at[0], gr.at[0], zp)

    def z_u(l):
        return send(wu_ref.at[l, theirs_h], ru.at[l], gs.at[1], gr.at[1], zp)

    CR = HB // 9

    def z_gate_up_part(l, k):
        j = k % 9
        src = pl.ds(pl.multiple_of((1 - z) * HB + j * CR, 16), CR)
        dst = pl.ds(pl.multiple_of(j * CR, 16), CR)

        @pl.when(k < 9)
        def _():
            send(wg_ref.at[l, src], rg.at[l, dst], gs.at[0], gr.at[0], zp).start()

        @pl.when(k >= 9)
        def _():
            send(wu_ref.at[l, src], ru.at[l, dst], gs.at[1], gr.at[1], zp).start()

    QR, OR = W // 8, QW // 8

    def z_attn_part(l, k):
        i = k // 2

        @pl.when(k % 2 == 0)
        def _():
            rows = pl.ds(pl.multiple_of(i * QR, 16), QR)
            send(wq_ref.at[l, rows], rq.at[l, rows], zs.at[0], zr.at[0], zp).start()
            send(wk_ref.at[l, rows], rk.at[l, rows], zs.at[1], zr.at[1], zp).start()
            send(wv_ref.at[l, rows], rv.at[l, rows], zs.at[2], zr.at[2], zp).start()

        @pl.when(k % 2 == 1)
        def _():
            rows = pl.ds(pl.multiple_of(i * OR, 16), OR)
            send(wo_ref.at[l, rows], ro.at[l, rows], zs.at[3], zr.at[3], zp).start()

    lo, hi = pl.ds(0, W), pl.ds(W, W)

    def ag_own(h, s, r, u):
        return (send(h.at[u, 0, q], h.at[u, 0, q], s.at[u, 0], r.at[u, 0], xp),
                send(h.at[u, 0, q], h.at[u, 0, q], s.at[u, 1], r.at[u, 1], yp))

    def ag_fwd(h, s, r, u):
        return (send(h.at[u, 0, qx, :, lo], h.at[u, 0, qx, :, lo], s.at[u, 2], r.at[u, 2], yp),
                send(h.at[u, 0, qy, :, hi], h.at[u, 0, qy, :, hi], s.at[u, 3], r.at[u, 3], xp))

    def ag_sib(h, s, r, u):
        return send(h.at[u, 0], h.at[u, 1], s.at[u, 4], r.at[u, 4], sp)

    def ag_send_own(h, s, r, u):
        for d in ag_own(h, s, r, u):
            d.start()

    def ag_fwd1(h, s, r, u):
        own_x, own_y = ag_own(h, s, r, u)
        fwd_y, fwd_x = ag_fwd(h, s, r, u)
        own_x.wait_recv()
        fwd_y.start()
        own_y.wait_recv()
        fwd_x.start()

    def ag_fwd2(h, s, r, u):
        fwd_y, fwd_x = ag_fwd(h, s, r, u)
        fwd_y.wait_recv()
        fwd_x.wait_recv()
        ag_sib(h, s, r, u).start()

    def ag_local(h, u):
        return pltpu.make_async_copy(h.at[u], hv.at[u % 2], hvs.at[u % 2])

    def ag_load(h, s, r, u):
        ag_sib(h, s, r, u).wait_recv()
        ag_local(h, u).start()

    def ag_finish(h, s, r, u):
        ag_local(h, u).wait()
        for d in ag_own(h, s, r, u) + ag_fwd(h, s, r, u) + (ag_sib(h, s, r, u),):
            d.wait_send()

    def h_store(h, u, i, j):
        return pltpu.make_async_copy(hst.at[i, j], h.at[u, 0, q], loc.at[i, j])

    def rs_d(u):
        return send(psib.at[u % 2], rd.at[u % 2], ds.at[u % 2], dr.at[u % 2], sp)

    def rs_x(u):
        i = u % 4
        return send(pown.at[i, :, 1 - x, :, pl.ds(0, V)], rx.at[i], xs.at[i], xr.at[i], xp)

    def rs_y(u):
        i = u % 4
        return send(pown.at[i, 1 - y, :, :, pl.ds(V, V)], ry.at[i], ys.at[i], yr.at[i], yp)

    def rs_x2(u):
        i = u % 4
        return send(t2.at[i, 1 - x], rx2.at[i], x2s.at[i], x2r.at[i], xp)

    def rs_y2(u):
        i = u % 4
        return send(t1.at[i, 1 - y], ry2.at[i], y2s.at[i], y2r.at[i], yp)

    def store_product(u, pairs):
        half = W // 2
        for j in range(2):
            cols = pl.ds(j * half, half)
            acc = None
            for a, w, rows in pairs:
                wv_ = w[:, cols] if rows is None else w[rows, cols]
                p = jnp.dot(a, wv_, preferred_element_type=F32)
                acc = p if acc is None else acc + p
            pown[u % 4, :, :, :, cols] = acc[: R // 2].reshape(2, 2, T, half)
            psib[u % 2, :, :, :, cols] = acc[R // 2:].reshape(2, 2, T, half)

    def rs_stage2(u):
        rs_d(u).wait()
        pown[u % 4] = pown[u % 4] + rd[u % 2]

    def rs_stage3(u):
        i = u % 4
        rs_x(u).wait()
        rs_y(u).wait()
        t1[i] = pown[i, :, x, :, pl.ds(0, V)] + rx[i]
        t2[i] = pown[i, y, :, :, pl.ds(V, V)] + ry[i]

    def rs_stage4(u):
        i = u % 4
        rs_x2(u).wait()
        rs_y2(u).wait()
        return t1[i, y] + ry2[i], t2[i, x] + rx2[i]

    def rs_steps(k, n, finish):
        @pl.when(jnp.logical_and(k >= LD, k < n + LD))
        def _():
            rs_stage2(k - LD)

        @pl.when(jnp.logical_and(k >= LD + LX, k < n + LD + LX))
        def _():
            rs_stage3(k - LD - LX)

        @pl.when(jnp.logical_and(k >= LT, k < n + LT))
        def _():
            finish(k - LT, *rs_stage4(k - LT))

    def rs_sends(k, n):
        @pl.when(jnp.logical_and(k >= 0, k < n))
        def _():
            rs_d(k).start()

        @pl.when(jnp.logical_and(k >= LD, k < n + LD))
        def _():
            rs_x(k - LD).start()
            rs_y(k - LD).start()

        @pl.when(jnp.logical_and(k >= LD + LX, k < n + LD + LX))
        def _():
            rs_x2(k - LD - LX).start()
            rs_y2(k - LD - LX).start()

    def m_send(b):
        return send(xbuf.at[b], mpeer.at[b], ms.at[b], mr.at[b], zp)

    def out_send(b):
        return send(mpeer.at[b, :, mine], xbuf.at[b, :, mine], os_.at[b], or_.at[b], zp)

    def hid_send(u):
        i = u % 4
        return send(hown.at[i], hrecv.at[i], hs.at[i], hr.at[i], zp)

    for d in (z_q(0), z_k(0), z_v(0), z_o(0)):
        d.start()
    first = [pltpu.make_async_copy(x_ref, xbuf, wl.at[0]),
             pltpu.make_async_copy(cos_ref.at[:, c], cbuf.at[0], wl.at[1]),
             pltpu.make_async_copy(cos_ref.at[:, 1 - c], cbuf.at[1], wl.at[2]),
             pltpu.make_async_copy(sin_ref.at[:, c], sbuf.at[0], wl.at[3]),
             pltpu.make_async_copy(sin_ref.at[:, 1 - c], sbuf.at[1], wl.at[4])]
    for d in first:
        d.start()
    for d in first:
        d.wait()

    def first_rows(b, carry):
        hst[b % 2, 0] = _norm(xbuf[b], ga_ref[0])
        d = h_store(ha.at[0], b, b % 2, 0)
        d.start()
        d.wait()
        ag_send_own(ha.at[0], sa, ra, b)
        return carry

    lax.fori_loop(0, NB, first_rows, 0)

    def pos_of(r):
        return 2 * T * ((r // T) % 4) + T * ((c + r // (4 * T)) % 2) + r % T

    def loop_a(l, wa_o, wa_r, wo_o, wo_r, o_all):
        h = ha.at[l]
        hbl = hb.at[l]
        loads = [pltpu.make_async_copy(wq_ref.at[l], wa_o.at[:, pl.ds(0, QW)], wl.at[0]),
                 pltpu.make_async_copy(wk_ref.at[l], wa_o.at[:, pl.ds(QW, HD)], wl.at[1]),
                 pltpu.make_async_copy(wv_ref.at[l], wa_o.at[:, pl.ds(QW + HD, HD)], wl.at[2]),
                 pltpu.make_async_copy(wo_ref.at[l], wo_o, wl.at[3])]
        for d in loads:
            d.start()
        ag_fwd1(h, sa, ra, 0)
        ag_fwd1(h, sa, ra, 1)
        ag_fwd2(h, sa, ra, 0)
        ag_load(h, sa, ra, 0)
        for d in (z_q(l), z_k(l), z_v(l)):
            d.wait()
        more = [pltpu.make_async_copy(rq.at[l], wa_r.at[:, pl.ds(0, QW)], wl.at[4]),
                pltpu.make_async_copy(rk.at[l], wa_r.at[:, pl.ds(QW, HD)], wl.at[5]),
                pltpu.make_async_copy(rv.at[l], wa_r.at[:, pl.ds(QW + HD, HD)], wl.at[6])]
        for d in more:
            d.start()
        for d in loads + more:
            d.wait()

        def finish(u, low, high):
            b = u % NB
            off = (z + (u // NB) * (1 - 2 * z)) * W
            ca = pl.ds(pl.multiple_of(off, 128), V)
            cb = pl.ds(pl.multiple_of(off + V, 128), V)
            xbuf[b, :, ca] = (xbuf[b, :, ca].astype(F32) + low).astype(BF16)
            xbuf[b, :, cb] = (xbuf[b, :, cb].astype(F32) + high).astype(BF16)

        def step(k, carry):
            @pl.when(k + 2 < NB)
            def _():
                ag_fwd1(h, sa, ra, k + 2)

            @pl.when(k + 1 < NB)
            def _():
                ag_fwd2(h, sa, ra, k + 1)

            @pl.when(k < NB)
            def _():
                ag_finish(h, sa, ra, k)
                i = k % 2
                acc = jnp.dot(hv[i, :, :, :, mine].reshape(R, W), wa_o[...], preferred_element_type=F32)
                acc += jnp.dot(hv[i, :, :, :, other].reshape(R, W), wa_r[...], preferred_element_type=F32)
                qkv = acc.astype(BF16)
                cosv = cbuf[...].reshape(R, HD)
                sinv = sbuf[...].reshape(R, HD)

                def rope(t):
                    t = t.astype(F32)
                    return (t * cosv + pltpu.roll(t, HD // 2, 1) * sinv).astype(BF16)

                mask = pos_of(lax.broadcasted_iota(jnp.int32, (R, R), 0)) >= pos_of(
                    lax.broadcasted_iota(jnp.int32, (R, R), 1))
                kk = rope(qkv[:, QW:QW + HD])
                vv = qkv[:, QW + HD:]
                for g in range(QW // HD):
                    s = lax.dot_general(rope(qkv[:, g * HD:(g + 1) * HD]), kk, NT, preferred_element_type=F32)
                    s = jnp.where(mask, s * HD ** -0.5, -jnp.inf)
                    e = jnp.exp(s - jnp.max(s, axis=-1, keepdims=True))
                    p = (e / jnp.sum(e, axis=-1, keepdims=True)).astype(BF16)
                    o_all[k, :, g * HD:(g + 1) * HD] = jnp.dot(p, vv, preferred_element_type=F32).astype(BF16)
                store_product(k, [(o_all[k], wo_o, None)])

            @pl.when(k == NB)
            def _():
                z_o(l).wait()
                d = pltpu.make_async_copy(ro.at[l], wo_r, wl.at[7])
                d.start()
                d.wait()

            @pl.when(jnp.logical_and(k >= NB, k < NU))
            def _():
                store_product(k, [(o_all[k - NB], wo_r, None)])

            rs_steps(k, NU, finish)

            @pl.when(k + 1 < NB)
            def _():
                ag_load(h, sa, ra, k + 1)

            rs_sends(k, NU)

            k0 = NB + LT

            @pl.when(jnp.logical_and(k >= k0, k < k0 + NB))
            def _():
                b = k - k0
                hst[b % 2, 0] = _norm(xbuf[b], gm_ref[l])
                h_store(hbl, 2 * b + z, b % 2, 0).start()
                m_send(b).start()

            @pl.when(jnp.logical_and(k >= k0 + 1, k < k0 + 1 + NB))
            def _():
                b = k - k0 - 1
                h_store(hbl, 2 * b + z, b % 2, 0).wait()
                ag_send_own(hbl, sb, rb, 2 * b + z)
                m_send(b).wait()
                hst[b % 2, 1] = _norm(mpeer[b], gm_ref[l])
                h_store(hbl, 2 * b + 1 - z, b % 2, 1).start()

            @pl.when(jnp.logical_and(k >= k0 + 2, k < k0 + 2 + NB))
            def _():
                b = k - k0 - 2
                h_store(hbl, 2 * b + 1 - z, b % 2, 1).wait()
                ag_send_own(hbl, sb, rb, 2 * b + 1 - z)

            @pl.when(k < 18)
            def _():
                z_gate_up_part(l, k)

            return carry

        lax.fori_loop(0, NU + LT + 2, step, 0)

    def loop_b(l, g_o, g_r, u_o, u_r, wd_v):
        h = hb.at[l]
        mine_h = pl.ds(pl.multiple_of(z * HB, 16), HB)
        loads = [pltpu.make_async_copy(wg_ref.at[l, mine_h], g_o, wl.at[0]),
                 pltpu.make_async_copy(wu_ref.at[l, mine_h], u_o, wl.at[1]),
                 pltpu.make_async_copy(wd_ref.at[l], wd_v, wl.at[2])]
        for d in loads:
            d.start()
        ag_fwd1(h, sb, rb, 0)
        ag_fwd1(h, sb, rb, 1)
        ag_fwd2(h, sb, rb, 0)
        ag_load(h, sb, rb, 0)
        for d in (z_g(l), z_u(l)):
            d.wait()
        more = [pltpu.make_async_copy(rg.at[l], g_r, wl.at[3]),
                pltpu.make_async_copy(ru.at[l], u_r, wl.at[4])]
        for d in more:
            d.start()
        for d in loads + more:
            d.wait()

        def finish(s, low, high):
            b = s // 2
            ca = pl.ds(pl.multiple_of(z * W, 128), V)
            cb = pl.ds(pl.multiple_of(z * W + V, 128), V)

            @pl.when(s % 2 == z)
            def _():
                xbuf[b, :, ca] = (xbuf[b, :, ca].astype(F32) + low).astype(BF16)
                xbuf[b, :, cb] = (xbuf[b, :, cb].astype(F32) + high).astype(BF16)

            @pl.when(s % 2 == 1 - z)
            def _():
                mpeer[b, :, ca] = (mpeer[b, :, ca].astype(F32) + low).astype(BF16)
                mpeer[b, :, cb] = (mpeer[b, :, cb].astype(F32) + high).astype(BF16)

        def step(k, carry):
            @pl.when(k + 2 < NU)
            def _():
                ag_fwd1(h, sb, rb, k + 2)

            @pl.when(k + 1 < NU)
            def _():
                ag_fwd2(h, sb, rb, k + 1)

            @pl.when(k < NU)
            def _():
                ag_finish(h, sb, rb, k)
                i = k % 2
                hm = hv[i, :, :, :, mine].reshape(R, W)
                ho = hv[i, :, :, :, other].reshape(R, W)
                gate = lax.dot_general(hm, g_o[...], NT, preferred_element_type=F32)
                gate += lax.dot_general(ho, g_r[...], NT, preferred_element_type=F32)
                up = lax.dot_general(hm, u_o[...], NT, preferred_element_type=F32)
                up += lax.dot_general(ho, u_r[...], NT, preferred_element_type=F32)
                hown[k % 4] = (jax.nn.silu(gate) * up).astype(BF16)

            v = k - LH

            @pl.when(jnp.logical_and(v >= 0, v < NU))
            def _():
                hid_send(v).wait()
                store_product(v, [(hown[v % 4], wd_v, mine_h), (hrecv[v % 4], wd_v, theirs_h)])

            rs_steps(v, NU, finish)

            @pl.when(k + 1 < NU)
            def _():
                ag_load(h, sb, rb, k + 1)

            @pl.when(k < NU)
            def _():
                hid_send(k).start()

            rs_sends(v, NU)

            s = v - LT

            @pl.when(jnp.logical_and(jnp.logical_and(s >= 0, s < NU), s % 2 == 1 - z))
            def _():
                out_send(s // 2).start()

            @pl.when(jnp.logical_and(jnp.logical_and(s >= 2, s < NU + 2), s % 2 == 0))
            def _():
                b = s // 2 - 1
                out_send(b).wait()

                @pl.when(l + 1 < n_layers)
                def _():
                    hst[b % 2, 0] = _norm(xbuf[b], ga_ref[(l + 1) % n_layers])
                    h_store(ha.at[(l + 1) % n_layers], b, b % 2, 0).start()

            @pl.when(jnp.logical_and(l + 1 < n_layers, jnp.logical_and(jnp.logical_and(s >= 3, s < NU + 3), s % 2 == 1)))
            def _():
                b = s // 2 - 1
                h_store(ha.at[(l + 1) % n_layers], b, b % 2, 0).wait()
                ag_send_own(ha.at[(l + 1) % n_layers], sa, ra, b)

            @pl.when(jnp.logical_and(l + 1 < n_layers, k < 16))
            def _():
                z_attn_part((l + 1) % n_layers, k)

            return carry

        lax.fori_loop(0, NU + LH + LT + 2, step, 0)

    def layer(l, carry):
        pl.run_scoped(
            functools.partial(loop_a, l),
            pltpu.VMEM((W, QW + 2 * HD), BF16), pltpu.VMEM((W, QW + 2 * HD), BF16),
            pltpu.VMEM((QW, W), BF16), pltpu.VMEM((QW, W), BF16), pltpu.VMEM((NB, R, QW), BF16))
        pl.run_scoped(
            functools.partial(loop_b, l),
            pltpu.VMEM((HB, W), BF16), pltpu.VMEM((HB, W), BF16),
            pltpu.VMEM((HB, W), BF16), pltpu.VMEM((HB, W), BF16), pltpu.VMEM((2 * HB, W), BF16))
        return carry

    lax.fori_loop(0, n_layers, layer, 0)
    d = pltpu.make_async_copy(xbuf, y_ref, wl.at[0])
    d.start()
    d.wait()


def solution(mesh):
    act_spec = P("fsdp", "model", None)
    col_spec = P(None, "fsdp", "model")
    row_spec = P(None, "model", "fsdp")

    def device_step(x_in, gain_attn, gain_mlp, rope_cos, rope_sin, w_q, w_k, w_v, w_o, w_gate, w_up, w_down):
        L = w_q.shape[0]
        NB, T, D = x_in.shape
        W, V = D // 2, D // 4
        HB = w_gate.shape[2] // 2
        NU, R = 2 * NB, 8 * T
        half = rope_cos.shape[1]
        cos2 = jnp.concatenate([rope_cos, rope_cos], axis=1).reshape(4, 2, T, 2 * half)
        sin2 = jnp.concatenate([-rope_sin, rope_sin], axis=1).reshape(4, 2, T, 2 * half)
        hbm = pl.BlockSpec(memory_space=pl.ANY)
        vmem = pl.BlockSpec(memory_space=pltpu.VMEM)
        dma = pltpu.SemaphoreType.DMA
        sds = jax.ShapeDtypeStruct
        outs = pl.pallas_call(
            _kernel,
            name="two_layers",
            in_specs=[hbm, vmem, vmem] + [hbm] * 9,
            out_specs=[hbm] * 9,
            out_shape=[
                sds(x_in.shape, BF16), sds(w_q.shape, BF16), sds(w_k.shape, BF16), sds(w_v.shape, BF16),
                sds(w_o.shape, BF16), sds((L, HB, W), BF16), sds((L, HB, W), BF16),
                sds((L, NB, 2, 4, T, D), BF16), sds((L, NU, 2, 4, T, D), BF16)],
            scratch_shapes=[
                pltpu.VMEM((NB, T, D), BF16), pltpu.VMEM((NB, T, D), BF16), pltpu.VMEM((2, 2, T, D), BF16),
                pltpu.VMEM((2, 2, 4, T, D), BF16),
                pltpu.VMEM((4, 2, 2, T, W), F32), pltpu.VMEM((2, 2, 2, T, W), F32), pltpu.VMEM((2, 2, 2, T, W), F32),
                pltpu.VMEM((4, 2, T, V), F32), pltpu.VMEM((4, 2, T, V), F32),
                pltpu.VMEM((4, 2, T, V), F32), pltpu.VMEM((4, 2, T, V), F32),
                pltpu.VMEM((4, T, V), F32), pltpu.VMEM((4, T, V), F32),
                pltpu.VMEM((4, R, HB), BF16), pltpu.VMEM((4, R, HB), BF16),
                pltpu.VMEM((2, 4, T, 2 * half), F32), pltpu.VMEM((2, 4, T, 2 * half), F32),
                dma((4,)), dma((4,)), dma((2,)), dma((2,)), dma((2,)), dma((2,)),
                dma((4,)), dma((4,)), dma((4,)), dma((4,)), dma((4,)), dma((4,)), dma((4,)), dma((4,)),
                dma((NB,)), dma((NB,)), dma((NB,)), dma((NB,)), dma((4,)), dma((4,)),
                dma((NB, 5)), dma((NB, 5)), dma((NU, 5)), dma((NU, 5)), dma((2, 2)), dma((2,)), dma((8,))],
            compiler_params=pltpu.CompilerParams(
                collective_id=0, has_side_effects=True, vmem_limit_bytes=67_000_000),
        )(x_in, gain_attn[:, None], gain_mlp[:, None], cos2, sin2, w_q, w_k, w_v, w_o,
          jnp.swapaxes(w_gate, 1, 2), jnp.swapaxes(w_up, 1, 2), w_down)
        return outs[0]

    return jax.shard_map(
        device_step, mesh=mesh,
        in_specs=(act_spec, P(), P(), P(), P(), col_spec, col_spec, col_spec, row_spec, col_spec, col_spec, row_spec),
        out_specs=act_spec, check_vma=False)
```

```python
import functools

import jax
import jax.numpy as jnp
from jax import lax
from jax.experimental import pallas as pl
from jax.experimental.pallas import tpu as pltpu
from jax.sharding import PartitionSpec as P

EPS = 1e-5
MESH = pl.DeviceIdType.MESH
NT = (((1,), (1,)), ((), ()))
LD = 1
LX = 2
LT = LD + 2 * LX
LH = 2
F32 = jnp.float32
BF16 = jnp.bfloat16


def _norm(rows, gain):
    rows = rows.astype(F32)
    mean_sq = jnp.mean(rows * rows, axis=-1, keepdims=True)
    return (rows * lax.rsqrt(mean_sq + EPS) * gain).astype(BF16)


def _kernel(
    x_ref, ga_ref, gm_ref, cos_ref, sin_ref, wq_ref, wk_ref, wv_ref, wo_ref, wg_ref, wu_ref, wd_ref,
    y_ref, rq, rk, rv, ro, rg, ru, ha, hb,
    xbuf, mpeer, hst, hv, pown, psib, rd, t1, t2, rx, ry, rx2, ry2, hown, hrecv, cbuf, sbuf, tmp,
    zs, zr, gs, gr, ds, dr, xs, xr, ys, yr, x2s, x2r, y2s, y2r, ms, mr, os_, or_, hs, hr,
    sa, ra, sb, rb, loc, hvs, wl,
):
    n_layers = wq_ref.shape[0]
    NB, T, D = x_ref.shape
    W, V = D // 2, D // 4
    QW = wq_ref.shape[2]
    HD = wk_ref.shape[2]
    HB = wg_ref.shape[1] // 2
    R = 8 * T
    NU = 2 * NB

    z = lax.axis_index("fsdp")
    m = lax.axis_index("model")
    y, x, c, q = m // 4, (m // 2) % 2, m % 2, m // 2
    qx, qy, qd = q + 1 - 2 * x, q + 2 - 4 * y, 3 - q
    zp, xp, yp, sp = (1 - z, m), (z, m + 2 - 4 * x), (z, m + 4 - 8 * y), (z, m + 1 - 2 * c)
    mine = pl.ds(pl.multiple_of(z * W, 128), W)
    other = pl.ds(pl.multiple_of((1 - z) * W, 128), W)

    barrier = pltpu.get_barrier_semaphore()
    for dev in (zp, xp, yp, sp):
        pl.semaphore_signal(barrier, inc=1, device_id=dev, device_id_type=MESH)
    pl.semaphore_wait(barrier, 4)

    def send(src, dst, s, r, dev):
        return pltpu.make_async_remote_copy(
            src_ref=src, dst_ref=dst, send_sem=s, recv_sem=r, device_id=dev, device_id_type=MESH)

    def z_q(l):
        return send(wq_ref.at[l], rq.at[l], zs.at[0], zr.at[0], zp)

    def z_k(l):
        return send(wk_ref.at[l], rk.at[l], zs.at[1], zr.at[1], zp)

    def z_v(l):
        return send(wv_ref.at[l], rv.at[l], zs.at[2], zr.at[2], zp)

    def z_o(l):
        return send(wo_ref.at[l], ro.at[l], zs.at[3], zr.at[3], zp)

    theirs_h = pl.ds(pl.multiple_of((1 - z) * HB, 16), HB)

    def z_g(l):
        return send(wg_ref.at[l, theirs_h], rg.at[l], gs.at[0], gr.at[0], zp)

    def z_u(l):
        return send(wu_ref.at[l, theirs_h], ru.at[l], gs.at[1], gr.at[1], zp)

    CR = HB // 9

    def z_gate_up_part(l, k):
        j = k % 9
        src = pl.ds(pl.multiple_of((1 - z) * HB + j * CR, 16), CR)
        dst = pl.ds(pl.multiple_of(j * CR, 16), CR)

        @pl.when(k < 9)
        def _():
            send(wg_ref.at[l, src], rg.at[l, dst], gs.at[0], gr.at[0], zp).start()

        @pl.when(k >= 9)
        def _():
            send(wu_ref.at[l, src], ru.at[l, dst], gs.at[1], gr.at[1], zp).start()

    QR, OR = W // 8, QW // 8

    def z_qkv_part(l, i):
        rows = pl.ds(pl.multiple_of(i * QR, 16), QR)
        send(wq_ref.at[l, rows], rq.at[l, rows], zs.at[0], zr.at[0], zp).start()
        send(wk_ref.at[l, rows], rk.at[l, rows], zs.at[1], zr.at[1], zp).start()
        send(wv_ref.at[l, rows], rv.at[l, rows], zs.at[2], zr.at[2], zp).start()

    def z_o_part(l, i):
        rows = pl.ds(pl.multiple_of(i * OR, 16), OR)
        send(wo_ref.at[l, rows], ro.at[l, rows], zs.at[3], zr.at[3], zp).start()

    lo, hi = pl.ds(0, W), pl.ds(W, W)

    def ag_own(h, s, r, u):
        return (send(h.at[u, 0, q], h.at[u, 0, q], s.at[u, 0], r.at[u, 0], xp),
                send(h.at[u, 0, q], h.at[u, 0, q], s.at[u, 1], r.at[u, 1], yp))

    def ag_fwd(h, s, r, u):
        return (send(h.at[u, 0, qx, :, lo], h.at[u, 0, qx, :, lo], s.at[u, 2], r.at[u, 2], yp),
                send(h.at[u, 0, qy, :, hi], h.at[u, 0, qy, :, hi], s.at[u, 3], r.at[u, 3], xp))

    def ag_sib(h, s, r, u):
        return send(h.at[u, 0], h.at[u, 1], s.at[u, 4], r.at[u, 4], sp)

    def ag_send_own(h, s, r, u):
        for d in ag_own(h, s, r, u):
            d.start()

    def ag_fwd1(h, s, r, u):
        own_x, own_y = ag_own(h, s, r, u)
        fwd_y, fwd_x = ag_fwd(h, s, r, u)
        own_x.wait_recv()
        fwd_y.start()
        own_y.wait_recv()
        fwd_x.start()

    def ag_fwd2(h, s, r, u):
        fwd_y, fwd_x = ag_fwd(h, s, r, u)
        fwd_y.wait_recv()
        fwd_x.wait_recv()
        ag_sib(h, s, r, u).start()

    def ag_local(h, u):
        return pltpu.make_async_copy(h.at[u], hv.at[u % 2], hvs.at[u % 2])

    def ag_load(h, s, r, u):
        ag_sib(h, s, r, u).wait_recv()
        ag_local(h, u).start()

    def ag_finish(h, s, r, u):
        ag_local(h, u).wait()
        for d in ag_own(h, s, r, u) + ag_fwd(h, s, r, u) + (ag_sib(h, s, r, u),):
            d.wait_send()

    def h_store(h, u, i, j):
        return pltpu.make_async_copy(hst.at[i, j], h.at[u, 0, q], loc.at[i, j])

    def rs_d(u):
        return send(psib.at[u % 2], rd.at[u % 2], ds.at[u % 2], dr.at[u % 2], sp)

    def rs_x(u):
        i = u % 4
        return send(pown.at[i, :, 1 - x, :, pl.ds(0, V)], rx.at[i], xs.at[i], xr.at[i], xp)

    def rs_y(u):
        i = u % 4
        return send(pown.at[i, 1 - y, :, :, pl.ds(V, V)], ry.at[i], ys.at[i], yr.at[i], yp)

    def rs_x2(u):
        i = u % 4
        return send(t2.at[i, 1 - x], rx2.at[i], x2s.at[i], x2r.at[i], xp)

    def rs_y2(u):
        i = u % 4
        return send(t1.at[i, 1 - y], ry2.at[i], y2s.at[i], y2r.at[i], yp)

    def store_product(u, pairs):
        half = W // 2
        for j in range(2):
            cols = pl.ds(j * half, half)
            acc = None
            for a, w, rows in pairs:
                wv_ = w[:, cols] if rows is None else w[rows, cols]
                p = jnp.dot(a, wv_, preferred_element_type=F32)
                acc = p if acc is None else acc + p
            pown[u % 4, :, :, :, cols] = acc[: R // 2].reshape(2, 2, T, half)
            psib[u % 2, :, :, :, cols] = acc[R // 2:].reshape(2, 2, T, half)

    def rs_stage2(u):
        rs_d(u).wait()
        pown[u % 4] = pown[u % 4] + rd[u % 2]

    def rs_stage3(u):
        i = u % 4
        rs_x(u).wait()
        rs_y(u).wait()
        t1[i] = pown[i, :, x, :, pl.ds(0, V)] + rx[i]
        t2[i] = pown[i, y, :, :, pl.ds(V, V)] + ry[i]

    def rs_stage4(u):
        i = u % 4
        rs_x2(u).wait()
        rs_y2(u).wait()
        return t1[i, y] + ry2[i], t2[i, x] + rx2[i]

    def rs_steps(k, n, finish):
        @pl.when(jnp.logical_and(k >= LD, k < n + LD))
        def _():
            rs_stage2(k - LD)

        @pl.when(jnp.logical_and(k >= LD + LX, k < n + LD + LX))
        def _():
            rs_stage3(k - LD - LX)

        @pl.when(jnp.logical_and(k >= LT, k < n + LT))
        def _():
            finish(k - LT, *rs_stage4(k - LT))

    def rs_sends(k, n):
        @pl.when(jnp.logical_and(k >= 0, k < n))
        def _():
            rs_d(k).start()

        @pl.when(jnp.logical_and(k >= LD, k < n + LD))
        def _():
            rs_x(k - LD).start()
            rs_y(k - LD).start()

        @pl.when(jnp.logical_and(k >= LD + LX, k < n + LD + LX))
        def _():
            rs_x2(k - LD - LX).start()
            rs_y2(k - LD - LX).start()

    def m_send(b):
        return send(xbuf.at[b], mpeer.at[b], ms.at[b], mr.at[b], zp)

    def out_send(b):
        return send(mpeer.at[b, :, mine], xbuf.at[b, :, mine], os_.at[b], or_.at[b], zp)

    def hid_send(u):
        i = u % 4
        return send(hown.at[i], hrecv.at[i], hs.at[i], hr.at[i], zp)

    for d in (z_q(0), z_k(0), z_v(0), z_o(0)):
        d.start()
    first = [pltpu.make_async_copy(x_ref, xbuf, wl.at[0])]
    for d in first:
        d.start()
    for d in first:
        d.wait()

    def first_rows(b, carry):
        hst[b % 2, 0] = _norm(xbuf[b], ga_ref[pl.ds(0, 1), :])
        d = h_store(ha.at[0], b, b % 2, 0)
        d.start()
        d.wait()
        ag_send_own(ha.at[0], sa, ra, b)
        return carry

    lax.fori_loop(0, NB, first_rows, 0)

    def first_forward(i, carry):
        ag_fwd1(ha.at[0], sa, ra, i)

        @pl.when(i >= 1)
        def _():
            ag_fwd2(ha.at[0], sa, ra, i - 1)

        return carry

    for ref, buf, sign in ((cos_ref, cbuf, 1.0), (sin_ref, sbuf, -1.0)):
        tab = ref[...].T
        tmp[...] = jnp.concatenate([sign * tab, tab], axis=1).reshape(4, 2, T, HD)
        buf[0] = tmp[:, c]
        buf[1] = tmp[:, 1 - c]

    lax.fori_loop(0, NB - 1, first_forward, 0)

    def when(*conds):
        c_ = conds[0]
        for d_ in conds[1:]:
            c_ = jnp.logical_and(c_, d_)
        return pl.when(c_)

    def pass_m(l, k):
        h = hb.at[l]

        def at(lag):
            if l == 0:
                q_ = k - lag - (NB + LT)
                return q_, jnp.logical_and(q_ >= 0, q_ < NB)
            q_ = k - lag - 5 - LT
            late = q_ > 8
            b_ = jnp.where(late, q_ - 4, q_ // 2)
            ok = jnp.logical_and(jnp.logical_and(q_ >= 0, q_ < 12), jnp.logical_or(late, q_ % 2 == 0))
            return b_, ok

        b0, ok0 = at(0)

        @pl.when(ok0)
        def _():
            hst[b0 % 2, 0] = _norm(xbuf[b0], gm_ref[pl.ds(l, 1), :])
            h_store(h, 2 * b0 + z, b0 % 2, 0).start()
            m_send(b0).start()

        b1, ok1 = at(1)

        @pl.when(ok1)
        def _():
            h_store(h, 2 * b1 + z, b1 % 2, 0).wait()
            ag_send_own(h, sb, rb, 2 * b1 + z)

        b3, ok3 = at(3)

        @pl.when(ok3)
        def _():
            h_store(h, 2 * b3 + 1 - z, b3 % 2, 1).wait()
            ag_send_own(h, sb, rb, 2 * b3 + 1 - z)

        b2, ok2 = at(2)

        @pl.when(ok2)
        def _():
            m_send(b2).wait()
            hst[b2 % 2, 1] = _norm(mpeer[b2], gm_ref[pl.ds(l, 1), :])
            h_store(h, 2 * b2 + 1 - z, b2 % 2, 1).start()

        b5, ok5 = at(5)

        @pl.when(ok5)
        def _():
            ag_fwd1(h, sb, rb, 2 * b5)
            ag_fwd1(h, sb, rb, 2 * b5 + 1)

        b7, ok7 = at(7)

        @pl.when(ok7)
        def _():
            ag_fwd2(h, sb, rb, 2 * b7)
            ag_fwd2(h, sb, rb, 2 * b7 + 1)

    def pass_y(l, s):
        @when(s >= 0, s < NU, s % 2 == 1 - z)
        def _():
            out_send(s // 2).start()

        last = l + 1 == n_layers

        @when(s >= 2, s < NU + 2, s % 2 == 0)
        def _():
            b = s // 2 - 1
            out_send(b).wait()
            if not last:
                hst[b % 2, 2] = _norm(xbuf[b], ga_ref[pl.ds(l + 1, 1), :])
                h_store(ha.at[l + 1], b, b % 2, 2).start()

        if not last:
            h = ha.at[l + 1]

            @when(s >= 3, s < NU + 3, s % 2 == 1)
            def _():
                b = s // 2 - 1
                h_store(h, b, b % 2, 2).wait()
                ag_send_own(h, sa, ra, b)

            @when(s >= 5, s < NU + 5, s % 2 == 1)
            def _():
                ag_fwd1(h, sa, ra, s // 2 - 2)

            @when(s >= 7, s < NU + 7, s % 2 == 1)
            def _():
                ag_fwd2(h, sa, ra, s // 2 - 3)

    def finish_y(s, low, high):
        b = s // 2
        ca = pl.ds(pl.multiple_of(z * W, 128), V)
        cb = pl.ds(pl.multiple_of(z * W + V, 128), V)

        @pl.when(s % 2 == z)
        def _():
            xbuf[b, :, ca] = (xbuf[b, :, ca].astype(F32) + low).astype(BF16)
            xbuf[b, :, cb] = (xbuf[b, :, cb].astype(F32) + high).astype(BF16)

        @pl.when(s % 2 == 1 - z)
        def _():
            mpeer[b, :, ca] = (mpeer[b, :, ca].astype(F32) + low).astype(BF16)
            mpeer[b, :, cb] = (mpeer[b, :, cb].astype(F32) + high).astype(BF16)

    def a_steps(l):
        return NU if l == 0 else NU + 1

    def a_unit(l, k):
        if l == 0:
            return k % NB, k, jnp.logical_and(k >= 0, k < NB), jnp.logical_and(k >= NB, k < NU)
        own = jnp.logical_and(k >= 0, jnp.logical_or(k < 3, jnp.logical_and(k % 2 == 0, k <= 12)))
        oth = jnp.logical_and(k >= 5, jnp.logical_or(jnp.logical_and(k % 2 == 1, k <= 13),
                                                     jnp.logical_and(k >= 14, k <= NU)))
        b_own = jnp.where(k < 3, k, (k + 2) // 2)
        b_oth = jnp.where(k < 14, (k - 5) // 2, k - 9)
        return jnp.where(own, b_own, b_oth), jnp.where(k < 4, k, k - 1), own, oth

    def a_stages(l, k):
        def at(lag):
            b, u, own, oth = a_unit(l, k - lag)
            return b, u, own, jnp.logical_or(own, oth)

        _, u2, _, ok2 = at(LD)
        pl.when(ok2)(lambda: rs_stage2(u2))
        _, u3, _, ok3 = at(LD + LX)
        pl.when(ok3)(lambda: rs_stage3(u3))
        b, u4, own4, ok4 = at(LT)

        @pl.when(ok4)
        def _():
            low, high = rs_stage4(u4)

            def add(col):
                ca = pl.ds(pl.multiple_of(col, 128), V)
                cb = pl.ds(pl.multiple_of(col + V, 128), V)
                xbuf[b, :, ca] = (xbuf[b, :, ca].astype(F32) + low).astype(BF16)
                xbuf[b, :, cb] = (xbuf[b, :, cb].astype(F32) + high).astype(BF16)

            pl.when(own4)(lambda: add(z * W))
            pl.when(jnp.logical_not(own4))(lambda: add((1 - z) * W))

    def a_sends(l, k):
        def at(lag):
            _, u, own, oth = a_unit(l, k - lag)
            return u, jnp.logical_or(own, oth)

        u1, ok1 = at(0)
        pl.when(ok1)(lambda: rs_d(u1).start())
        u2, ok2 = at(LD)

        @pl.when(ok2)
        def _():
            rs_x(u2).start()
            rs_y(u2).start()

        u3, ok3 = at(LD + LX)

        @pl.when(ok3)
        def _():
            rs_x2(u3).start()
            rs_y2(u3).start()

    def gap(l):
        return 8 if l == 0 else 2

    def b_steps(l):
        return gap(l) + LH + NU

    def pos_of(r):
        return 2 * T * ((r // T) % 4) + T * ((c + r // (4 * T)) % 2) + r % T

    def attend(l, k, b, h, wa_o, wa_r, wo_o, o_all):
        ag_finish(h, sa, ra, b)
        i = b % 2
        acc = jnp.dot(hv[i, :, :, :, mine].reshape(R, W), wa_o[...], preferred_element_type=F32)
        acc += jnp.dot(hv[i, :, :, :, other].reshape(R, W), wa_r[...], preferred_element_type=F32)
        qkv = acc.astype(BF16)
        cosv = cbuf[...].reshape(R, HD)
        sinv = sbuf[...].reshape(R, HD)

        def rope(t):
            t = t.astype(F32)
            return (t * cosv + pltpu.roll(t, HD // 2, 1) * sinv).astype(BF16)

        mask = pos_of(lax.broadcasted_iota(jnp.int32, (R, R), 0)) >= pos_of(
            lax.broadcasted_iota(jnp.int32, (R, R), 1))
        kk = rope(qkv[:, QW:QW + HD])
        vv = qkv[:, QW + HD:]
        for g in range(QW // HD):
            sc = lax.dot_general(rope(qkv[:, g * HD:(g + 1) * HD]), kk, NT, preferred_element_type=F32)
            sc = jnp.where(mask, sc * HD ** -0.5, -jnp.inf)
            e = jnp.exp(sc - jnp.max(sc, axis=-1, keepdims=True))
            p = (e / jnp.sum(e, axis=-1, keepdims=True)).astype(BF16)
            o_all[b, :, g * HD:(g + 1) * HD] = jnp.dot(p, vv, preferred_element_type=F32).astype(BF16)

    def loop_a(l, wa_o, wa_r, wo_o, wo_r, o_all):
        h = ha.at[l]
        loads = [pltpu.make_async_copy(wq_ref.at[l], wa_o.at[:, pl.ds(0, QW)], wl.at[0]),
                 pltpu.make_async_copy(wk_ref.at[l], wa_o.at[:, pl.ds(QW, HD)], wl.at[1]),
                 pltpu.make_async_copy(wv_ref.at[l], wa_o.at[:, pl.ds(QW + HD, HD)], wl.at[2]),
                 pltpu.make_async_copy(wo_ref.at[l], wo_o, wl.at[3])]
        for d in loads:
            d.start()
        ag_load(h, sa, ra, 0)
        for d in (z_q(l), z_k(l), z_v(l)):
            d.wait()
        more = [pltpu.make_async_copy(rq.at[l], wa_r.at[:, pl.ds(0, QW)], wl.at[4]),
                pltpu.make_async_copy(rk.at[l], wa_r.at[:, pl.ds(QW, HD)], wl.at[5]),
                pltpu.make_async_copy(rv.at[l], wa_r.at[:, pl.ds(QW + HD, HD)], wl.at[6])]
        for d in more:
            d.start()
        for d in loads + more:
            d.wait()
        first_other = NB if l == 0 else 5

        def step(k, carry):
            if l == 0:
                @pl.when(k == 0)
                def _():
                    ag_fwd1(h, sa, ra, NB - 1)

                @pl.when(k < 2)
                def _():
                    ag_fwd2(h, sa, ra, NB - 2 + k)

            b, u, own, oth = a_unit(l, k)

            @pl.when(own)
            def _():
                attend(l, k, b, h, wa_o, wa_r, wo_o, o_all)
                store_product(u, [(o_all[b], wo_o, None)])

            @pl.when(k == first_other)
            def _():
                z_o(l).wait()
                d = pltpu.make_async_copy(ro.at[l], wo_r, wl.at[7])
                d.start()
                d.wait()

            @pl.when(oth)
            def _():
                store_product(u, [(o_all[b], wo_r, None)])

            if l > 0:
                rs_steps(NU + k, NU, finish_y)
            a_stages(l, k)
            if l > 0:
                rs_sends(NU + k, NU)
            a_sends(l, k)
            if l > 0:
                pass_y(l - 1, NU + k - LT)
            pass_m(l, k)

            bn, _, own_next, _ = a_unit(l, k + 1)

            @pl.when(own_next)
            def _():
                ag_load(h, sa, ra, bn)

            if l == 0:
                @pl.when(k >= 8)
                def _():
                    z_gate_up_part(l, k - 8)
            else:
                @pl.when(k < 4)
                def _():
                    z_o_part(l, 4 + k)

                @when(k >= 4, k < 7)
                def _():
                    z_gate_up_part(l, 2 * (k - 4))
                    z_gate_up_part(l, 2 * (k - 4) + 1)

                @pl.when(k >= 7)
                def _():
                    z_gate_up_part(l, k - 1)

            return carry

        lax.fori_loop(0, a_steps(l), step, 0)

    def loop_b(l, g_o, g_r, u_o, u_r, wd_v):
        h = hb.at[l]
        mine_h = pl.ds(pl.multiple_of(z * HB, 16), HB)
        j0 = gap(l)
        loads = [pltpu.make_async_copy(wg_ref.at[l, mine_h], g_o, wl.at[0]),
                 pltpu.make_async_copy(wu_ref.at[l, mine_h], u_o, wl.at[1]),
                 pltpu.make_async_copy(wd_ref.at[l], wd_v, wl.at[2])]
        more = [pltpu.make_async_copy(rg.at[l], g_r, wl.at[3]),
                pltpu.make_async_copy(ru.at[l], u_r, wl.at[4])]
        for d in loads:
            d.start()

        def step(k, carry):
            @pl.when(k == j0)
            def _():
                for d in (z_g(l), z_u(l)):
                    d.wait()
                for d in more:
                    d.start()
                for d in loads + more:
                    d.wait()

            @when(k >= j0, k < j0 + NU)
            def _():
                u = k - j0
                ag_finish(h, sb, rb, u)
                i = u % 2
                hm = hv[i, :, :, :, mine].reshape(R, W)
                ho = hv[i, :, :, :, other].reshape(R, W)
                gate = lax.dot_general(hm, g_o[...], NT, preferred_element_type=F32)
                gate += lax.dot_general(ho, g_r[...], NT, preferred_element_type=F32)
                up = lax.dot_general(hm, u_o[...], NT, preferred_element_type=F32)
                up += lax.dot_general(ho, u_r[...], NT, preferred_element_type=F32)
                hown[u % 4] = (jax.nn.silu(gate) * up).astype(BF16)

            v = k - j0 - LH

            @pl.when(v >= 0)
            def _():
                hid_send(v).wait()
                store_product(v, [(hown[v % 4], wd_v, mine_h), (hrecv[v % 4], wd_v, theirs_h)])

            a_stages(l, a_steps(l) + k)
            rs_steps(v, NU, finish_y)

            @when(k >= j0, k < j0 + NU)
            def _():
                hid_send(k - j0).start()

            a_sends(l, a_steps(l) + k)
            rs_sends(v, NU)
            pass_m(l, a_steps(l) + k)
            pass_y(l, v - LT)

            @when(k >= j0 - 1, k < j0 + NU - 1)
            def _():
                ag_load(h, sb, rb, k - j0 + 1)

            if l == 0:
                @pl.when(k < 5)
                def _():
                    z_gate_up_part(l, 8 + k)

                @pl.when(k == 5)
                def _():
                    z_gate_up_part(l, 13)
                    z_gate_up_part(l, 14)

                @pl.when(k == 6)
                def _():
                    z_gate_up_part(l, 15)
                    z_gate_up_part(l, 16)
                    z_gate_up_part(l, 17)
            else:
                @pl.when(k < 2)
                def _():
                    z_gate_up_part(l, 16 + k)
            if l + 1 < n_layers:
                @pl.when(k == 7)
                def _():
                    z_qkv_part(l + 1, 0)

                @when(k >= 8, k <= 20, k % 2 == 0)
                def _():
                    z_qkv_part(l + 1, (k - 6) // 2)

                @pl.when(k >= 22)
                def _():
                    z_o_part(l + 1, k - 22)

            return carry

        lax.fori_loop(0, b_steps(l), step, 0)

    for l in range(n_layers):
        pl.run_scoped(
            functools.partial(loop_a, l),
            pltpu.VMEM((W, QW + 2 * HD), BF16), pltpu.VMEM((W, QW + 2 * HD), BF16),
            pltpu.VMEM((QW, W), BF16), pltpu.VMEM((QW, W), BF16), pltpu.VMEM((NB, R, QW), BF16))
        pl.run_scoped(
            functools.partial(loop_b, l),
            pltpu.VMEM((HB, W), BF16), pltpu.VMEM((HB, W), BF16),
            pltpu.VMEM((HB, W), BF16), pltpu.VMEM((HB, W), BF16), pltpu.VMEM((2 * HB, W), BF16))

    def tail(v, carry):
        rs_steps(v, NU, finish_y)
        rs_sends(v, NU)
        pass_y(n_layers - 1, v - LT)
        return carry

    lax.fori_loop(NU, NU + LT + 2, tail, 0)
    d = pltpu.make_async_copy(xbuf, y_ref, wl.at[0])
    d.start()
    d.wait()


def solution(mesh):
    act_spec = P("fsdp", "model", None)
    col_spec = P(None, "fsdp", "model")
    row_spec = P(None, "model", "fsdp")

    def device_step(x_in, gain_attn, gain_mlp, rope_cos, rope_sin, w_q, w_k, w_v, w_o, w_gate, w_up, w_down):
        L = w_q.shape[0]
        NB, T, D = x_in.shape
        W, V = D // 2, D // 4
        HB = w_gate.shape[2] // 2
        NU, R = 2 * NB, 8 * T
        half = rope_cos.shape[1]
        hbm = pl.BlockSpec(memory_space=pl.ANY)
        vmem = pl.BlockSpec(memory_space=pltpu.VMEM)
        dma = pltpu.SemaphoreType.DMA
        sds = jax.ShapeDtypeStruct
        outs = pl.pallas_call(
            _kernel,
            name="two_layers",
            in_specs=[hbm] + [vmem] * 4 + [hbm] * 7,
            out_specs=[hbm] * 9,
            out_shape=[
                sds(x_in.shape, BF16), sds(w_q.shape, BF16), sds(w_k.shape, BF16), sds(w_v.shape, BF16),
                sds(w_o.shape, BF16), sds((L, HB, W), BF16), sds((L, HB, W), BF16),
                sds((L, NB, 2, 4, T, D), BF16), sds((L, NU, 2, 4, T, D), BF16)],
            scratch_shapes=[
                pltpu.VMEM((NB, T, D), BF16), pltpu.VMEM((NB, T, D), BF16), pltpu.VMEM((2, 3, T, D), BF16),
                pltpu.VMEM((2, 2, 4, T, D), BF16),
                pltpu.VMEM((4, 2, 2, T, W), F32), pltpu.VMEM((2, 2, 2, T, W), F32), pltpu.VMEM((2, 2, 2, T, W), F32),
                pltpu.VMEM((4, 2, T, V), F32), pltpu.VMEM((4, 2, T, V), F32),
                pltpu.VMEM((4, 2, T, V), F32), pltpu.VMEM((4, 2, T, V), F32),
                pltpu.VMEM((4, T, V), F32), pltpu.VMEM((4, T, V), F32),
                pltpu.VMEM((4, R, HB), BF16), pltpu.VMEM((4, R, HB), BF16),
                pltpu.VMEM((2, 4, T, 2 * half), F32), pltpu.VMEM((2, 4, T, 2 * half), F32),
                pltpu.VMEM((4, 2, T, 2 * half), F32),
                dma((4,)), dma((4,)), dma((2,)), dma((2,)), dma((2,)), dma((2,)),
                dma((4,)), dma((4,)), dma((4,)), dma((4,)), dma((4,)), dma((4,)), dma((4,)), dma((4,)),
                dma((NB,)), dma((NB,)), dma((NB,)), dma((NB,)), dma((4,)), dma((4,)),
                dma((NB, 5)), dma((NB, 5)), dma((NU, 5)), dma((NU, 5)), dma((2, 3)), dma((2,)), dma((8,))],
            compiler_params=pltpu.CompilerParams(
                collective_id=0, has_side_effects=True, vmem_limit_bytes=67_000_000),
        )(x_in, gain_attn, gain_mlp, rope_cos.T, rope_sin.T, w_q, w_k, w_v, w_o,
          jnp.swapaxes(w_gate, 1, 2), jnp.swapaxes(w_up, 1, 2), w_down)
        return outs[0]

    return jax.shard_map(
        device_step, mesh=mesh,
        in_specs=(act_spec, P(), P(), P(), P(), col_spec, col_spec, col_spec, row_spec, col_spec, col_spec, row_spec),
        out_specs=act_spec, check_vma=False)
```

```python
import functools

import jax
import jax.numpy as jnp
from jax import lax
from jax.experimental import pallas as pl
from jax.experimental.pallas import tpu as pltpu
from jax.sharding import PartitionSpec as P

EPS = 1e-5
MESH = pl.DeviceIdType.MESH
NN = (((1,), (0,)), ((), ()))
NT = (((1,), (1,)), ((), ()))
TN = (((0,), (0,)), ((), ()))
LD = 1
LX = 2
LT = LD + 2 * LX
LH = 2
LM = (2, 2)
GAP = (8, 6)
SLOTS, CHIPS, CORES, PAIR = 4, 4, 2, 2
ALIGN, LANES = 16, 128
SEMS = "442222444444448888444433" + "22888"
GU, ATTN = 9, 8

CUT_A = (20, 38)
CUT_B = (22, 16)
CUTS = 40

ATTEND = ("01234567--------", "012-3-4-5-6-7-------")
OWN = ("01234567--------", "--012-3-4-5-6-7-----")
OTHER = ("--------01234567", "---------0-1-2-34567")
GU_IN_A = ("0000001111111111", "00010220211000111111")
GU_IN_B = ("111122", "1011")
QKV_IN_B = ("000000011010101010101", "")
O_IN_A = ("", "1211")
O_IN_B = ("00000000000000000000000012", "")
F32 = jnp.float32
BF16 = jnp.bfloat16


def _norm(rows, gain):
    rows = rows.astype(F32)
    mean_sq = jnp.mean(rows * rows, axis=-1, keepdims=True)
    return (rows * lax.rsqrt(mean_sq + EPS) * gain).astype(BF16)


def _kernel(
    x_ref, ga_ref, gm_ref, cos_ref, sin_ref, wq_ref, wk_ref, wv_ref, wo_ref, wg_ref, wu_ref, wd_ref,
    y_ref, rq, rk, rv, ro, rg, ru, ha, hb, rw, row,
    xbuf, mpeer, hst, hv, pown, psib, rd, t1, t2, rx, ry, rx2, ry2, hown, hrecv, cbuf, sbuf, tmp, ox, xres, mst,
    zs, zr, gs, gr, ds, dr, xs, xr, ys, yr, x2s, x2r, y2s, y2r, ms, mr, os_, or_, hs, hr, mxs, mxr, wxs, wxr,
    loc, hvs, wl, oxs, oxr, sa, ra, sb, rb, xrs, xrr,
):
    n_layers = wq_ref.shape[0]
    NB, T, D = x_ref.shape
    W, V = D // PAIR, D // CHIPS
    QW = wq_ref.shape[2]
    HD = wk_ref.shape[2]
    HB = wg_ref.shape[1] // PAIR
    R = CHIPS * CORES * T
    NU = PAIR * NB

    z = lax.axis_index("fsdp")
    m = lax.axis_index("model")
    y, x, c, q = m // 4, (m // 2) % 2, m % 2, m // 2
    qx, qy, qd = q + 1 - 2 * x, q + 2 - 4 * y, 3 - q
    zp, xp, yp, sp = (1 - z, m), (z, m + 2 - 4 * x), (z, m + 4 - 8 * y), (z, m + 1 - 2 * c)

    def lanes(start, size):
        return pl.ds(pl.multiple_of(start, LANES), size)

    def rows(start, size):
        return pl.ds(pl.multiple_of(start, ALIGN), size)

    mine, other = lanes(z * W, W), lanes((1 - z) * W, W)
    low_v, high_v = pl.ds(0, V), pl.ds(V, V)

    def even(i):
        return i % PAIR == 0

    def half_of(i):
        return i // PAIR

    def when(*conds):
        return pl.when(functools.reduce(jnp.logical_and, conds))

    def within(k, n):
        return jnp.logical_and(k >= 0, k < n)

    def lookup(table, k):
        runs = []
        for i in sorted(table):
            if runs:
                run = runs[-1]
                stride = i - run[-1]
                if table[i] == table[run[-1]] + 1 and stride in (1, PAIR) and (
                        len(run) == 1 or stride == run[-1] - run[-2]):
                    run.append(i)
                    continue
            runs.append([i])
        value, there = None, None
        for run in reversed(runs):
            first, last = run[0], run[-1]
            stride = run[1] - first if len(run) > 1 else 1
            ok = jnp.logical_and(k >= first, k <= last)
            if stride > 1:
                ok = jnp.logical_and(ok, (k - first) % stride == 0)
            val = (k - first) // stride + table[first]
            value = val if value is None else jnp.where(k <= last, val, value)
            there = ok if there is None else jnp.logical_or(there, ok)
        return value, there

    def table(text):
        return {i: int(ch) for i, ch in enumerate(text) if ch.isdigit()}

    def parts(texts, k, start):
        done = sum(int(ch) for text in texts[:-1] for ch in text)
        for i, ch in enumerate(texts[-1]):
            n = int(ch)
            if n:
                @pl.when(k == i)
                def _():
                    for j in range(done, done + n):
                        start(j)
            done += n

    barrier = pltpu.get_barrier_semaphore()
    for dev in (zp, xp, yp, sp):
        pl.semaphore_signal(barrier, inc=1, device_id=dev, device_id_type=MESH)
    pl.semaphore_wait(barrier, 4)

    def send(src, dst, s, r, dev):
        return pltpu.make_async_remote_copy(
            src_ref=src, dst_ref=dst, send_sem=s, recv_sem=r, device_id=dev, device_id_type=MESH)

    def z_q(l):
        return send(wq_ref.at[l], rq.at[l], zs.at[0], zr.at[0], zp)

    def z_k(l):
        return send(wk_ref.at[l], rk.at[l], zs.at[1], zr.at[1], zp)

    def z_v(l):
        return send(wv_ref.at[l], rv.at[l], zs.at[2], zr.at[2], zp)

    def z_o(l):
        return send(wo_ref.at[l], ro, zs.at[3], zr.at[3], zp)

    mine_h, theirs_h = rows(z * HB, HB), rows((1 - z) * HB, HB)

    def z_g(l):
        return send(wg_ref.at[l, theirs_h], rg.at[l], gs.at[0], gr.at[0], zp)

    def z_u(l):
        return send(wu_ref.at[l, theirs_h], ru.at[l], gs.at[1], gr.at[1], zp)

    def z_gate_up_part(l, j):
        size = HB // GU
        ref, out, i = (wg_ref, rg, 0) if j < GU else (wu_ref, ru, 1)
        at = (j % GU) * size
        send(ref.at[l, rows((1 - z) * HB + at, size)], out.at[l, pl.ds(at, size)], gs.at[i], gr.at[i], zp).start()

    def z_qkv_part(l, j):
        size = W // ATTN
        at = pl.ds(j * size, size)
        for i, (ref, out) in enumerate(((wq_ref, rq), (wk_ref, rk), (wv_ref, rv))):
            send(ref.at[l, at], out.at[l, at], zs.at[i], zr.at[i], zp).start()

    def z_o_part(l, j):
        size = QW // ATTN
        for d in z_oq(l, pl.ds(j * size, size)):
            d.start()

    def cut_of(share):
        return max(1, D // LANES * share // CUTS) * LANES

    def cut_a(l):
        return cut_of(CUT_A[l])

    def cut_b(l):
        return cut_of(CUT_B[l])

    def ag_own(h, s, r, u):
        own = h.at[u, 0, q]
        return [send(own, own, s.at[u, i], r.at[u, i], dev) for i, dev in enumerate((xp, yp))]

    def ag_fwd(h, s, r, u, cut):
        from_x, from_y = h.at[u, 0, qx, :, pl.ds(0, cut)], h.at[u, 0, qy, :, pl.ds(cut, D - cut)]
        return [send(from_x, from_x, s.at[u, 2], r.at[u, 2], yp), send(from_y, from_y, s.at[u, 3], r.at[u, 3], xp)]

    def ag_sib(h, s, r, u):
        return send(h.at[u, 0], h.at[u, 1], s.at[u, CHIPS], r.at[u, CHIPS], sp)

    def ag_send_own(h, s, r, u):
        for d in ag_own(h, s, r, u):
            d.start()

    def ag_fwd1(h, s, r, u, cut):
        for own, fwd in zip(ag_own(h, s, r, u), ag_fwd(h, s, r, u, cut)):
            own.wait_recv()
            fwd.start()

    def ag_fwd2(h, s, r, u, cut):
        for fwd in ag_fwd(h, s, r, u, cut):
            fwd.wait_recv()
        ag_sib(h, s, r, u).start()

    def ag_local(h, u):
        return pltpu.make_async_copy(h.at[u], hv.at[u % PAIR], hvs.at[u % PAIR])

    def ag_load(h, s, r, u):
        ag_sib(h, s, r, u).wait_recv()
        ag_local(h, u).start()

    def ag_finish(h, s, r, u, cut):
        ag_local(h, u).wait()
        for d in ag_own(h, s, r, u) + ag_fwd(h, s, r, u, cut) + [ag_sib(h, s, r, u)]:
            d.wait_send()

    def y_store(b):
        return pltpu.make_async_copy(xbuf.at[b], y_ref.at[b], oxs.at[b])

    def h_store(h, u, j):
        return pltpu.make_async_copy(hst.at[j], h.at[u, 0, q], loc.at[j])

    def rs_d(u):
        return send(psib.at[u % PAIR], rd.at[u % PAIR], ds.at[u % PAIR], dr.at[u % PAIR], sp)

    def rs_x(u):
        i = u % SLOTS
        return send(pown.at[i, :, 1 - x, :, low_v], rx.at[i], xs.at[i], xr.at[i], xp)

    def rs_y(u):
        i = u % SLOTS
        return send(pown.at[i, 1 - y, :, :, high_v], ry.at[i], ys.at[i], yr.at[i], yp)

    def ra_d(u):
        return send(psib.at[u % PAIR, :, :, :, low_v], rd.at[u % PAIR, :, :, :, low_v],
                    ds.at[u % PAIR], dr.at[u % PAIR], sp)

    def ra_y(u):
        i = u % SLOTS
        return send(pown.at[i, 1 - y, :, :, low_v], ry.at[i], ys.at[i], yr.at[i], yp)

    def ra_m(u, b, half):
        cols = lanes(half * W + x * V, V)
        return send(mst.at[u % (LH + 1)], xbuf.at[b, :, cols], mxs.at[u % SLOTS], mxr.at[u % SLOTS], xp)

    def o_send(o_all, b):
        return send(o_all.at[b], ox.at[b % (NB - 1)], oxs.at[b], oxr.at[b], xp)

    def res_send(b, half):
        src = lanes(half * W + (1 - x) * V, V)
        dst = lanes(half * V, V)
        return send(xbuf.at[b, :, src], xres.at[b, :, dst], xrs.at[b, half], xrr.at[b, half], xp)

    def w_send(l):
        cols = lanes((1 - x) * V, V)
        return send(wo_ref.at[l, :, cols], rw.at[...], wxs.at[0], wxr.at[0], xp)

    def z_oq(l, rows=slice(None)):
        cols = lanes(x * V, V)
        return (send(wo_ref.at[l, rows, cols], row.at[0, rows], wxs.at[1], wxr.at[1], zp),
                send(rw.at[rows], row.at[1, rows], wxs.at[2], wxr.at[2], zp))

    def rs_x2(u):
        i = u % SLOTS
        return send(t2.at[u % (LH + 1), 1 - x], rx2.at[i], x2s.at[i], x2r.at[i], xp)

    def rs_y2(u):
        i = u % SLOTS
        return send(t1.at[u % (LH + 1), 1 - y], ry2.at[i], y2s.at[i], y2r.at[i], yp)

    def store_product(u, pairs, width):
        half = W // 2
        for j in range(width // half):
            cols = pl.ds(j * half, half)
            acc = None
            for a, w, rows in pairs:
                wv_ = w[:, cols] if rows is None else w[rows, cols]
                p = lax.dot_general(a, wv_, TN if rows is not None else NN, preferred_element_type=F32)
                acc = p if acc is None else acc + p
            pown[u % SLOTS, :, :, :, cols] = acc[: R // 2].reshape(2, 2, T, half)
            psib[u % PAIR, :, :, :, cols] = acc[R // 2:].reshape(2, 2, T, half)

    def rs_stage2(u):
        rs_d(u).wait()
        pown[u % SLOTS] = pown[u % SLOTS] + rd[u % PAIR]

    def rs_stage3(u):
        i = u % SLOTS
        rs_x(u).wait()
        rs_y(u).wait()
        t1[u % (LH + 1)] = pown[i, :, x, :, low_v] + rx[i]
        t2[u % (LH + 1)] = pown[i, y, :, :, high_v] + ry[i]

    def rs_stage4(u):
        i = u % SLOTS
        rs_x2(u).wait()
        rs_y2(u).wait()
        return t1[u % (LH + 1), y] + ry2[i], t2[u % (LH + 1), x] + rx2[i]

    def rs_steps(k, n, finish):
        @pl.when(jnp.logical_and(k >= LD, k < n + LD))
        def _():
            rs_stage2(k - LD)

        @pl.when(jnp.logical_and(k >= LD + LX, k < n + LD + LX))
        def _():
            rs_stage3(k - LD - LX)

        @pl.when(jnp.logical_and(k >= LT, k < n + LT))
        def _():
            finish(k - LT, *rs_stage4(k - LT))

    def rs_sends(k, n):
        @pl.when(jnp.logical_and(k >= 0, k < n))
        def _():
            rs_d(k).start()

        @pl.when(jnp.logical_and(k >= LD, k < n + LD))
        def _():
            rs_x(k - LD).start()
            rs_y(k - LD).start()

        @pl.when(jnp.logical_and(k >= LD + LX, k < n + LD + LX))
        def _():
            rs_x2(k - LD - LX).start()
            rs_y2(k - LD - LX).start()

    def m_send(b):
        return send(xbuf.at[b], mpeer.at[b], ms.at[b], mr.at[b], zp)

    def out_send(b):
        return send(mpeer.at[b, :, mine], xbuf.at[b, :, mine], os_.at[b], or_.at[b], zp)

    def hid_send(u):
        i = u % SLOTS
        return send(hown.at[u % (LH + 1)], hrecv.at[i], hs.at[i], hr.at[i], zp)

    for d in (z_q(0), z_k(0), z_v(0), z_o(0)):
        d.start()
    first = [pltpu.make_async_copy(x_ref, xbuf, wl.at[0])]
    for d in first:
        d.start()
    for d in first:
        d.wait()

    def first_rows(b, carry):
        hst[0] = _norm(xbuf[b], ga_ref[pl.ds(0, 1), :])
        d = h_store(ha.at[0], b, 0)
        d.start()
        d.wait()
        ag_send_own(ha.at[0], sa, ra, b)
        return carry

    lax.fori_loop(0, NB, first_rows, 0)

    def first_forward(i, carry):
        ag_fwd1(ha.at[0], sa, ra, i, cut_a(0))

        @pl.when(i >= 1)
        def _():
            ag_fwd2(ha.at[0], sa, ra, i - 1, cut_a(0))

        return carry

    for ref, buf, sign in ((cos_ref, cbuf, 1.0), (sin_ref, sbuf, -1.0)):
        tab = ref[...].T
        tmp[...] = jnp.concatenate([sign * tab, tab], axis=1).reshape(4, 2, T, HD)
        buf[0] = tmp[:, c]
        buf[1] = tmp[:, 1 - c]

    lax.fori_loop(0, NB, first_forward, 0)
    w_send(1).start()
    def pass_m(l, k):
        h = hb.at[l]
        cut = cut_b(l)
        wait_m = LM[l]

        def at(lag, run):
            b, ok = lookup(table(OTHER[l]), k - lag - LT)
            pl.when(ok)(lambda: run(b))

        def own(b):
            return PAIR * b + z

        def theirs(b):
            return PAIR * b + 1 - z

        def send_own(b):
            h_store(h, own(b), 0).wait()
            ag_send_own(h, sb, rb, own(b))

        def start_own(b):
            hst[0] = _norm(xbuf[b], gm_ref[pl.ds(l, 1), :])
            h_store(h, own(b), 0).start()
            m_send(b).start()

        def send_theirs(b):
            h_store(h, theirs(b), 1).wait()
            ag_send_own(h, sb, rb, theirs(b))

        def start_theirs(b):
            m_send(b).wait()
            hst[1] = _norm(mpeer[b], gm_ref[pl.ds(l, 1), :])
            h_store(h, theirs(b), 1).start()

        def forward(b):
            for j in range(PAIR):
                ag_fwd1(h, sb, rb, PAIR * b + j, cut)

        def forward_more(b):
            for j in range(PAIR):
                ag_fwd2(h, sb, rb, PAIR * b + j, cut)

        at(1, send_own)
        at(0, start_own)
        at(wait_m + 1, send_theirs)
        at(wait_m, start_theirs)
        at(wait_m + LX + 1, forward)
        at(wait_m + LX + LX + 1, forward_more)

    def pass_y(l, s):
        last = l + 1 == n_layers

        @when(within(s, NU), s % PAIR == 1 - z)
        def _():
            out_send(half_of(s)).start()

        def at(lag, run):
            i = s - lag - 1
            when(within(i, NU), even(i))(lambda: run(half_of(i)))

        def got(b):
            out_send(b).wait()
            if last:
                y_store(b).start()
                return
            hst[0] = _norm(xbuf[b], ga_ref[pl.ds(l + 1, 1), :])
            h_store(ha.at[l + 1], b, 0).start()
            for half in range(PAIR):
                res_send(b, half).start()

        at(1, got)
        if not last:
            h, cut = ha.at[l + 1], cut_a(l + 1)

            def send_own(b):
                h_store(h, b, 0).wait()
                ag_send_own(h, sa, ra, b)

            at(LX, send_own)
            at(LX + LX, lambda b: ag_fwd1(h, sa, ra, b, cut))
            at(LX + LX + LX, lambda b: ag_fwd2(h, sa, ra, b, cut))

    def add(buf, b, start, low, high):
        for at, part in ((start, low), (start + V, high)):
            cols = lanes(at, V)
            buf[b, :, cols] = (buf[b, :, cols].astype(F32) + part).astype(BF16)

    def finish_y(s, low, high):
        b = half_of(s)
        pl.when(s % PAIR == z)(lambda: add(xbuf, b, z * W, low, high))
        pl.when(s % PAIR == 1 - z)(lambda: add(mpeer, b, z * W, low, high))

    def finish_m(u, low, high):
        half = z + (u // NB) * (1 - z - z)
        add(xbuf, u % NB, half * W, low, high)

    def a_steps(l):
        return len(ATTEND[l])

    def a_attend(l, k):
        return lookup(table(ATTEND[l]), k)

    def a_unit(l, k):
        own, oth = table(OWN[l]), table(OTHER[l])
        b_own, is_own = lookup(own, k)
        b_oth, is_oth = lookup(oth, k)
        u, _ = lookup({i: n for n, i in enumerate(sorted({**own, **oth}))}, k)
        return jnp.where(is_own, b_own, b_oth), u, is_own, is_oth

    def a_stages(l, k):
        if l == 0:
            rs_steps(k, NU, finish_m)
            return

        def at(lag):
            b, u, own, oth = a_unit(l, k - lag)
            half = jnp.where(own, z, 1 - z)
            return b, u, half, jnp.logical_or(own, oth)

        _, u2, _, ok2 = at(LD)

        @pl.when(ok2)
        def _():
            ra_d(u2).wait()
            cols = low_v
            pown[u2 % SLOTS, :, :, :, cols] = pown[u2 % SLOTS, :, :, :, cols] + rd[u2 % PAIR, :, :, :, cols]

        b3, u3, half3, ok3 = at(LD + LX)

        @pl.when(ok3)
        def _():
            i = u3 % SLOTS
            ra_y(u3).wait()
            res_send(b3, half3).wait_recv()
            cols = lanes(half3 * W + x * V, V)
            xbuf[b3, :, cols] = (xbuf[b3, :, cols].astype(F32)
                                 + (pown[i, y, x, :, low_v] + ry[i, x])).astype(BF16)
            res = xres[b3, :, lanes(half3 * V, V)].astype(F32)
            mst[u3 % (LH + 1)] = (res + (pown[i, y, 1 - x, :, low_v] + ry[i, 1 - x])).astype(BF16)

        b4, u4, half4, ok4 = at(LT)
        pl.when(ok4)(lambda: ra_m(u4, b4, half4).wait())

    def a_sends(l, k):
        if l == 0:
            rs_sends(k, NU)
            return

        def at(lag):
            b, u, own, oth = a_unit(l, k - lag)
            return b, u, jnp.where(own, z, 1 - z), jnp.logical_or(own, oth)

        _, u1, _, ok1 = at(0)
        pl.when(ok1)(lambda: ra_d(u1).start())
        _, u2, _, ok2 = at(LD)
        pl.when(ok2)(lambda: ra_y(u2).start())
        b3, u3, half3, ok3 = at(LD + LX)
        pl.when(ok3)(lambda: ra_m(u3, b3, half3).start())

    def b_steps(l):
        return GAP[l] + LH + NU

    def pos_of(r):
        rail = r // (CHIPS * T)
        return CORES * T * ((r // T) % CHIPS) + T * ((c + rail) % CORES) + r % T

    def attend(l, b, h, wa_o, wa_r, o_all):
        ag_finish(h, sa, ra, b, cut_a(l))
        i = b % PAIR
        acc = jnp.dot(hv[i, :, :, :, mine].reshape(R, W), wa_o[...], preferred_element_type=F32)
        acc += jnp.dot(hv[i, :, :, :, other].reshape(R, W), wa_r[...], preferred_element_type=F32)
        qkv = acc.astype(BF16)
        cosv = cbuf[...].reshape(R, HD)
        sinv = sbuf[...].reshape(R, HD)

        def rope(t):
            t = t.astype(F32)
            return (t * cosv + pltpu.roll(t, HD // 2, 1) * sinv).astype(BF16)

        mask = pos_of(lax.broadcasted_iota(jnp.int32, (R, R), 0)) >= pos_of(
            lax.broadcasted_iota(jnp.int32, (R, R), 1))
        kk = rope(qkv[:, QW:QW + HD])
        vv = qkv[:, QW + HD:]
        for g in range(QW // HD):
            sc = lax.dot_general(rope(qkv[:, g * HD:(g + 1) * HD]), kk, NT, preferred_element_type=F32)
            sc = jnp.where(mask, sc * HD ** -0.5, -jnp.inf)
            e = jnp.exp(sc - jnp.max(sc, axis=-1, keepdims=True))
            p = (e / jnp.sum(e, axis=-1, keepdims=True)).astype(BF16)
            o_all[b, :, g * HD:(g + 1) * HD] = jnp.dot(p, vv, preferred_element_type=F32).astype(BF16)

    def loop_a(l, wa_o, wa_r, w_own, w_oth, o_all):
        h = ha.at[l]
        my_v = lanes(x * V, V)
        loads = [pltpu.make_async_copy(wq_ref.at[l], wa_o.at[:, pl.ds(0, QW)], wl.at[0]),
                 pltpu.make_async_copy(wk_ref.at[l], wa_o.at[:, pl.ds(QW, HD)], wl.at[1]),
                 pltpu.make_async_copy(wv_ref.at[l], wa_o.at[:, pl.ds(QW + HD, HD)], wl.at[2]),
                 pltpu.make_async_copy(wo_ref.at[l] if l == 0 else wo_ref.at[l, :, my_v],
                                       w_own.at[0], wl.at[3])]
        if l > 0:
            loads.append(pltpu.make_async_copy(rw, w_own.at[1], wl.at[7]))
        for d in loads:
            d.start()
        ag_load(h, sa, ra, 0)
        for d in (z_q(l), z_k(l), z_v(l)):
            d.wait()
        more = [pltpu.make_async_copy(rq.at[l], wa_r.at[:, pl.ds(0, QW)], wl.at[4]),
                pltpu.make_async_copy(rk.at[l], wa_r.at[:, pl.ds(QW, HD)], wl.at[5]),
                pltpu.make_async_copy(rv.at[l], wa_r.at[:, pl.ds(QW + HD, HD)], wl.at[6])]
        for d in more:
            d.start()
        for d in loads + more:
            d.wait()
        first_other = min(table(OTHER[l]))

        def step(k, carry):
            if l == 0:
                @pl.when(k == 0)
                def _():
                    ag_fwd2(h, sa, ra, NB - 1, cut_a(0))

            bn, next_ok = a_attend(l, k + 1)
            pl.when(next_ok)(lambda: ag_load(h, sa, ra, bn))
            ba, ok = a_attend(l, k)
            pl.when(ok)(lambda: attend(l, ba, h, wa_o, wa_r, o_all))
            b, u, own, oth = a_unit(l, k)

            @pl.when(own)
            def _():
                if l == 0:
                    store_product(u, [(o_all[b], w_own.at[0], None)], W)
                else:
                    o_send(o_all, b).wait()
                    store_product(u, [(o_all[b], w_own.at[0], None), (ox[b % (NB - 1)], w_own.at[1], None)], V)

            @pl.when(k == first_other)
            def _():
                got = (z_o(l),) if l == 0 else z_oq(l)
                for d in got:
                    d.wait()
                if l == 0:
                    into = [pltpu.make_async_copy(ro, w_oth.at[0], wl.at[5])]
                else:
                    into = [pltpu.make_async_copy(row.at[i], w_oth.at[i], wl.at[5 + i]) for i in range(2)]
                for d in into:
                    d.start()
                for d in into:
                    d.wait()

            @pl.when(oth)
            def _():
                if l == 0:
                    store_product(u, [(o_all[b], w_oth.at[0], None)], W)
                else:
                    store_product(u, [(o_all[b], w_oth.at[0], None), (ox[b % (NB - 1)], w_oth.at[1], None)], V)

            if l > 0:
                rs_steps(NU + k, NU, finish_y)
            a_stages(l, k)
            if l > 0:
                rs_sends(NU + k, NU)
            if l > 0:
                @pl.when(ok)
                def _():
                    for half in range(2):
                        res_send(ba, half).wait_send()
                    o_send(o_all, ba).start()

            a_sends(l, k)
            if l > 0:
                pass_y(l - 1, NU + k - LT)
            pass_m(l, k)

            parts((O_IN_B[l - 1], O_IN_A[l]), k, functools.partial(z_o_part, l))
            parts((GU_IN_A[l],), k, functools.partial(z_gate_up_part, l))
            return carry

        lax.fori_loop(0, a_steps(l), step, 0)

    def loop_b(l, g_o, g_r, u_o, u_r, wd_v):
        h = hb.at[l]
        j0 = GAP[l]
        loads = [pltpu.make_async_copy(wg_ref.at[l, mine_h], g_o, wl.at[0]),
                 pltpu.make_async_copy(wu_ref.at[l, mine_h], u_o, wl.at[1]),
                 pltpu.make_async_copy(wd_ref.at[l], wd_v, wl.at[2])]
        more = [pltpu.make_async_copy(rg.at[l], g_r, wl.at[3]),
                pltpu.make_async_copy(ru.at[l], u_r, wl.at[4])]
        for d in loads:
            d.start()

        def step(k, carry):
            @pl.when(k == j0)
            def _():
                for d in (z_g(l), z_u(l)):
                    d.wait()
                for d in more:
                    d.start()
                for d in loads + more:
                    d.wait()

            @when(k >= j0 - 1, k < j0 + NU - 1)
            def _():
                ag_load(h, sb, rb, k - j0 + 1)

            @when(k >= j0, k < j0 + NU)
            def _():
                u = k - j0
                ag_finish(h, sb, rb, u, cut_b(l))
                i = u % PAIR
                hm = hv[i, :, :, :, mine].reshape(R, W)
                ho = hv[i, :, :, :, other].reshape(R, W)
                gate = lax.dot_general(g_o[...], hm, NT, preferred_element_type=F32)
                gate += lax.dot_general(g_r[...], ho, NT, preferred_element_type=F32)
                up = lax.dot_general(u_o[...], hm, NT, preferred_element_type=F32)
                up += lax.dot_general(u_r[...], ho, NT, preferred_element_type=F32)
                hown[u % (LH + 1)] = (jax.nn.silu(gate) * up).astype(BF16)

            v = k - j0 - LH

            @pl.when(v >= 0)
            def _():
                hid_send(v).wait()
                store_product(v, [(hown[v % (LH + 1)], wd_v, mine_h), (hrecv[v % SLOTS], wd_v, theirs_h)], W)

            a_stages(l, a_steps(l) + k)
            rs_steps(v, NU, finish_y)

            @when(k >= j0, k < j0 + NU)
            def _():
                hid_send(k - j0).start()

            a_sends(l, a_steps(l) + k)
            rs_sends(v, NU)
            pass_m(l, a_steps(l) + k)
            pass_y(l, v - LT)

            parts((GU_IN_A[l], GU_IN_B[l]), k, functools.partial(z_gate_up_part, l))
            if l + 1 < n_layers:
                @pl.when(k == min(table(O_IN_B[l].replace("0", "-"))))
                def _():
                    w_send(l + 1).wait()

                parts((QKV_IN_B[l],), k, functools.partial(z_qkv_part, l + 1))
                parts((O_IN_B[l],), k, functools.partial(z_o_part, l + 1))

            return carry

        lax.fori_loop(0, b_steps(l), step, 0)

    for l in range(n_layers):
        pl.run_scoped(
            functools.partial(loop_a, l),
            pltpu.VMEM((W, QW + 2 * HD), BF16), pltpu.VMEM((W, QW + 2 * HD), BF16),
            pltpu.VMEM((1, QW, W) if l == 0 else (2, QW, V), BF16),
            pltpu.VMEM((1, QW, W) if l == 0 else (2, QW, V), BF16), pltpu.VMEM((NB, R, QW), BF16))
        pl.run_scoped(
            functools.partial(loop_b, l),
            pltpu.VMEM((HB, W), BF16), pltpu.VMEM((HB, W), BF16),
            pltpu.VMEM((HB, W), BF16), pltpu.VMEM((HB, W), BF16), pltpu.VMEM((2 * HB, W), BF16))

    def tail(v, carry):
        rs_steps(v, NU, finish_y)
        rs_sends(v, NU)
        pass_y(n_layers - 1, v - LT)
        return carry

    lax.fori_loop(NU, NU + LT + 2, tail, 0)
    for b in range(NB):
        y_store(b).wait()


def solution(mesh):
    act_spec = P("fsdp", "model", None)
    col_spec = P(None, "fsdp", "model")
    row_spec = P(None, "model", "fsdp")

    def device_step(x_in, gain_attn, gain_mlp, rope_cos, rope_sin, w_q, w_k, w_v, w_o, w_gate, w_up, w_down):
        L, NB, T, D = w_q.shape[0], *x_in.shape
        W, V = D // PAIR, D // CHIPS
        HB = w_gate.shape[-1] // PAIR
        NU, R = PAIR * NB, CHIPS * CORES * T
        HD = PAIR * rope_cos.shape[-1]
        QW = w_o.shape[1]
        hbm = pl.BlockSpec(memory_space=pl.ANY)
        vmem = pl.BlockSpec(memory_space=pltpu.VMEM)
        sds = jax.ShapeDtypeStruct

        def buf(dtype, *shape):
            return pltpu.VMEM(shape, dtype)

        def sems(*shape):
            return pltpu.SemaphoreType.DMA(shape)

        args = (x_in, gain_attn, gain_mlp, rope_cos.T, rope_sin.T, w_q, w_k, w_v, w_o,
                jnp.swapaxes(w_gate, 1, -1), jnp.swapaxes(w_up, 1, -1), w_down)
        half_rows, plane_rows = (L, HB, W), (CORES, CHIPS, T, D)
        shapes = [x_in.shape, w_q.shape, w_k.shape, w_v.shape, w_o.shape[1:], half_rows, half_rows,
                  (L, NB) + plane_rows, (L, NU) + plane_rows, (QW, V), (PAIR, QW, V)]
        unit, hop = (PAIR, PAIR, T, W), (PAIR, T, V)
        in_flight, hidden, tables = LH + 1, (HB, R), (CORES, CHIPS, T, HD)
        outs = pl.pallas_call(
            _kernel,
            name="two_layers",
            in_specs=[vmem if a.ndim <= PAIR else hbm for a in args],
            out_specs=[hbm] * len(shapes),
            out_shape=[sds(shape, BF16) for shape in shapes],
            scratch_shapes=[
                buf(BF16, NB, T, D), buf(BF16, NB, T, D), buf(BF16, PAIR, T, D), buf(BF16, PAIR, *plane_rows),
                buf(F32, SLOTS, *unit), buf(F32, PAIR, *unit), buf(F32, PAIR, *unit),
                buf(F32, in_flight, *hop), buf(F32, in_flight, *hop), buf(F32, SLOTS, *hop), buf(F32, SLOTS, *hop),
                buf(F32, SLOTS, T, V), buf(F32, SLOTS, T, V), buf(BF16, in_flight, *hidden), buf(BF16, SLOTS, *hidden),
                buf(F32, *tables), buf(F32, *tables), buf(F32, CHIPS, CORES, T, HD),
                buf(BF16, NB - 1, R, QW), buf(BF16, NB, T, W), buf(BF16, in_flight, T, V)]
            + [sems(int(ch)) for ch in SEMS] + [sems(NB, CHIPS + 1), sems(NB, CHIPS + 1), sems(NU, CHIPS + 1),
                                                sems(NU, CHIPS + 1), sems(NB, PAIR), sems(NB, PAIR)],
            compiler_params=pltpu.CompilerParams(
                collective_id=0, has_side_effects=True, vmem_limit_bytes=67_000_000),
        )(*args)
        return outs[0]

    return jax.shard_map(
        device_step, mesh=mesh,
        in_specs=(act_spec, P(), P(), P(), P(), col_spec, col_spec, col_spec, row_spec, col_spec, col_spec, row_spec),
        out_specs=act_spec, check_vma=False)
```

```python
import functools

import jax
import jax.numpy as jnp
from jax import lax
from jax.experimental import pallas as pl
from jax.experimental.pallas import tpu as pltpu
from jax.sharding import PartitionSpec as P

EPS = 1e-5
MESH = pl.DeviceIdType.MESH
NN = (((1,), (0,)), ((), ()))
NT = (((1,), (1,)), ((), ()))
TN = (((0,), (0,)), ((), ()))
LD = 1
LX = 2
LT = LD + 2 * LX
LH = 2
LM = (7, 4)
LAGS_M = ((10, 12, 10, 12), (6, 9, 7, 9))
LAGS_Y = (4, 6)
FREE = 8
EXTRA = (6, 0)
PAIRED = (False, True)
GAP = (12, 8)
SLOTS, CHIPS, CORES, PAIR = 4, 4, 2, 2
ALIGN, LANES = 16, 128
SEMS = "4422224444444488884444" + "22888"
GU, ATTN = 18, 8

CUT_A = (25, 31)
CUT_B = (23, 19)
CUTS = 40

ATTEND = ("01234567--------", "01-234-5-6---7--------------")
OWN = ("01234567--------", "---012-34-5--6-7------------")
OTHER = ("--------01234567", "---------0--1-2-----3--456-7")
GU_IN_A = ("2000204222220012", "0201010040310002400022030032")
GU_IN_B = ("02122021212", "2022")
QKV_IN_B = ("000000000002000000000101000011200000", "")
O_IN_A = ("", "03")
O_IN_B = ("000000000000000000000000011000001011", "")
F32 = jnp.float32
BF16 = jnp.bfloat16


def _norm(rows, gain):
    rows = rows.astype(F32)
    mean_sq = jnp.mean(rows * rows, axis=-1, keepdims=True)
    return (rows * lax.rsqrt(mean_sq + EPS) * gain).astype(BF16)


def _kernel(
    x_ref, ga_ref, gm_ref, cos_ref, sin_ref, wq_ref, wk_ref, wv_ref, wo_ref, wg_ref, wu_ref, wd_ref,
    y_ref, rq, rk, rv, ro, rg, ru, ha, hb, rw, row,
    xbuf, mpeer, hst, hv, pown, psib, rd, t1, t2, rx, ry, rx2, ry2, hown, hrecv, cbuf, sbuf, tmp, ox, xres, mst,
    zs, zr, gs, gr, ds, dr, xs, xr, ys, yr, x2s, x2r, y2s, y2r, ms, mr, os_, or_, hs, hr, mxs, mxr,
    loc, hvs, wl, oxs, oxr, sa, ra, sb, rb, xrs, xrr, wxs, wxr,
):
    n_layers = wq_ref.shape[0]
    NB, T, D = x_ref.shape
    W, V = D // PAIR, D // CHIPS
    QW = wq_ref.shape[2]
    HD = wk_ref.shape[2]
    HB = wg_ref.shape[1] // PAIR
    R = CHIPS * CORES * T
    NU = PAIR * NB

    z = lax.axis_index("fsdp")
    m = lax.axis_index("model")
    y, x, c, q = m // 4, (m // 2) % 2, m % 2, m // 2
    qx, qy, qd = q + 1 - 2 * x, q + 2 - 4 * y, 3 - q
    zp, xp, yp, sp = (1 - z, m), (z, m + 2 - 4 * x), (z, m + 4 - 8 * y), (z, m + 1 - 2 * c)

    def lanes(start, size):
        return pl.ds(pl.multiple_of(start, LANES), size)

    def rows(start, size):
        return pl.ds(pl.multiple_of(start, ALIGN), size)

    mine, other = lanes(z * W, W), lanes((1 - z) * W, W)
    low_v, high_v = pl.ds(0, V), pl.ds(V, V)

    def even(i):
        return i % PAIR == 0

    def half_of(i):
        return i // PAIR

    def when(*conds):
        return pl.when(functools.reduce(jnp.logical_and, conds))

    def within(k, n):
        return jnp.logical_and(k >= 0, k < n)

    def lookup(table, k):
        runs = []
        for i in sorted(table):
            if runs:
                run = runs[-1]
                stride = i - run[-1]
                if table[i] == table[run[-1]] + 1 and stride in (1, PAIR) and (
                        len(run) == 1 or stride == run[-1] - run[-2]):
                    run.append(i)
                    continue
            runs.append([i])
        value, there = None, None
        for run in reversed(runs):
            first, last = run[0], run[-1]
            stride = run[1] - first if len(run) > 1 else 1
            ok = jnp.logical_and(k >= first, k <= last)
            if stride > 1:
                ok = jnp.logical_and(ok, (k - first) % stride == 0)
            val = (k - first) // stride + table[first]
            value = val if value is None else jnp.where(k <= last, val, value)
            there = ok if there is None else jnp.logical_or(there, ok)
        return value, there

    def table(text):
        return {i: int(ch) for i, ch in enumerate(text) if ch.isdigit()}

    def parts(texts, k, start):
        done = sum(int(ch) for text in texts[:-1] for ch in text)
        for i, ch in enumerate(texts[-1]):
            n = int(ch)
            if n:
                @pl.when(k == i)
                def _():
                    for j in range(done, done + n):
                        start(j)
            done += n

    barrier = pltpu.get_barrier_semaphore()
    for dev in (zp, xp, yp, sp):
        pl.semaphore_signal(barrier, inc=1, device_id=dev, device_id_type=MESH)
    pl.semaphore_wait(barrier, 4)

    def send(src, dst, s, r, dev):
        return pltpu.make_async_remote_copy(
            src_ref=src, dst_ref=dst, send_sem=s, recv_sem=r, device_id=dev, device_id_type=MESH)

    def z_q(l):
        return send(wq_ref.at[l], rq.at[l], zs.at[0], zr.at[0], zp)

    def z_k(l):
        return send(wk_ref.at[l], rk.at[l], zs.at[1], zr.at[1], zp)

    def z_v(l):
        return send(wv_ref.at[l], rv.at[l], zs.at[2], zr.at[2], zp)

    def z_o(l):
        return send(wo_ref.at[l], ro, zs.at[3], zr.at[3], zp)

    mine_h, theirs_h = rows(z * HB, HB), rows((1 - z) * HB, HB)

    def z_g(l):
        return send(wg_ref.at[l, theirs_h], rg.at[l], gs.at[0], gr.at[0], zp)

    def z_u(l):
        return send(wu_ref.at[l, theirs_h], ru.at[l], gs.at[1], gr.at[1], zp)

    def z_gate_up_part(l, j):
        size = HB // GU
        ref, out, i = (wg_ref, rg, 0) if j < GU else (wu_ref, ru, 1)
        at = (j % GU) * size
        send(ref.at[l, rows((1 - z) * HB + at, size)], out.at[l, pl.ds(at, size)], gs.at[i], gr.at[i], zp).start()

    def z_qkv_part(l, j):
        size = W // ATTN
        at = pl.ds(j * size, size)
        for i, (ref, out) in enumerate(((wq_ref, rq), (wk_ref, rk), (wv_ref, rv))):
            send(ref.at[l, at], out.at[l, at], zs.at[i], zr.at[i], zp).start()

    def z_o_part(l, j):
        size = QW // ATTN
        for d in z_oq(l, pl.ds(j * size, size)):
            d.start()

    def cut_of(share):
        return max(1, D // LANES * share // CUTS) * LANES

    def cut_a(l):
        return cut_of(CUT_A[l])

    def cut_b(l):
        return cut_of(CUT_B[l])

    def ag_own(h, s, r, u):
        own = h.at[u, 0, q]
        return [send(own, own, s.at[u, i], r.at[u, i], dev) for i, dev in enumerate((xp, yp))]

    def ag_fwd(h, s, r, u, cut):
        from_x, from_y = h.at[u, 0, qx, :, pl.ds(0, cut)], h.at[u, 0, qy, :, pl.ds(cut, D - cut)]
        return [send(from_x, from_x, s.at[u, 2], r.at[u, 2], yp), send(from_y, from_y, s.at[u, 3], r.at[u, 3], xp)]

    def ag_sib(h, s, r, u):
        return send(h.at[u, 0], h.at[u, 1], s.at[u, CHIPS], r.at[u, CHIPS], sp)

    def ag_send_own(h, s, r, u):
        for d in ag_own(h, s, r, u):
            d.start()

    def ag_fwd1(h, s, r, u, cut):
        for own, fwd in zip(ag_own(h, s, r, u), ag_fwd(h, s, r, u, cut)):
            own.wait_recv()
            fwd.start()

    def ag_fwd2(h, s, r, u, cut):
        for fwd in ag_fwd(h, s, r, u, cut):
            fwd.wait_recv()
        ag_sib(h, s, r, u).start()

    def ag_local(h, u):
        return pltpu.make_async_copy(h.at[u], hv.at[u % PAIR], hvs.at[u % PAIR])

    def ag_load(h, s, r, u):
        ag_sib(h, s, r, u).wait_recv()
        ag_local(h, u).start()

    def ag_finish(h, s, r, u, cut):
        ag_local(h, u).wait()
        for d in ag_own(h, s, r, u) + ag_fwd(h, s, r, u, cut) + [ag_sib(h, s, r, u)]:
            d.wait_send()

    def y_store(b):
        return pltpu.make_async_copy(xbuf.at[b], y_ref.at[b], oxs.at[b])

    def h_store(h, u, j):
        return pltpu.make_async_copy(hst.at[j], h.at[u, 0, q], loc.at[j])

    def rs_d(u):
        return send(psib.at[u % PAIR], rd.at[u % PAIR], ds.at[u % PAIR], dr.at[u % PAIR], sp)

    def rs_x(u):
        i = u % SLOTS
        return send(pown.at[i, :, 1 - x, :, low_v], rx.at[i], xs.at[i], xr.at[i], xp)

    def rs_y(u):
        i = u % SLOTS
        return send(pown.at[i, 1 - y, :, :, high_v], ry.at[i], ys.at[i], yr.at[i], yp)

    def ra_d(u):
        return send(psib.at[u % PAIR, :, :, :, low_v], rd.at[u % PAIR, :, :, :, low_v],
                    ds.at[u % PAIR], dr.at[u % PAIR], sp)

    def ra_y(u):
        i = u % SLOTS
        return send(pown.at[i, 1 - y, :, :, low_v], ry.at[i], ys.at[i], yr.at[i], yp)

    def ra_m(u, b, half):
        cols = lanes(half * W + x * V, V)
        return send(mst.at[u % (LH + 1)], xbuf.at[b, :, cols], mxs.at[u % SLOTS], mxr.at[u % SLOTS], xp)

    def o_send(o_all, b):
        return send(o_all.at[b], ox.at[b % (NB - 1)], oxs.at[b], oxr.at[b], xp)

    def res_send(b, half):
        src = lanes(half * W + (1 - x) * V, V)
        dst = lanes(half * V, V)
        return send(xbuf.at[b, :, src], xres.at[b, :, dst], xrs.at[b, half], xrr.at[b, half], xp)

    def w_send(l):
        cols = lanes((1 - x) * V, V)
        return send(wo_ref.at[l, :, cols], rw.at[l], wxs.at[l, 0], wxr.at[l, 0], xp)

    def z_oq(l, rows=slice(None)):
        cols = lanes(x * V, V)
        return (send(wo_ref.at[l, rows, cols], row.at[l, 0, rows], wxs.at[l, 1], wxr.at[l, 1], zp),
                send(rw.at[l, rows], row.at[l, 1, rows], wxs.at[l, 2], wxr.at[l, 2], zp))

    def rs_x2(u):
        i = u % SLOTS
        return send(t2.at[u % (LH + 1), 1 - x], rx2.at[i], x2s.at[i], x2r.at[i], xp)

    def rs_y2(u):
        i = u % SLOTS
        return send(t1.at[u % (LH + 1), 1 - y], ry2.at[i], y2s.at[i], y2r.at[i], yp)

    def store_product(u, pairs, width):
        half = W // 2
        for j in range(width // half):
            cols = pl.ds(j * half, half)
            acc = None
            for a, w, rows in pairs:
                wv_ = w[:, cols] if rows is None else w[rows, cols]
                p = lax.dot_general(a, wv_, TN if rows is not None else NN, preferred_element_type=F32)
                acc = p if acc is None else acc + p
            pown[u % SLOTS, :, :, :, cols] = acc[: R // 2].reshape(2, 2, T, half)
            psib[u % PAIR, :, :, :, cols] = acc[R // 2:].reshape(2, 2, T, half)

    def rs_stage2(u):
        rs_d(u).wait()
        pown[u % SLOTS] = pown[u % SLOTS] + rd[u % PAIR]

    def rs_stage3(u):
        i = u % SLOTS
        rs_x(u).wait()
        rs_y(u).wait()
        t1[u % (LH + 1)] = pown[i, :, x, :, low_v] + rx[i]
        t2[u % (LH + 1)] = pown[i, y, :, :, high_v] + ry[i]

    def rs_stage4(u):
        i = u % SLOTS
        rs_x2(u).wait()
        rs_y2(u).wait()
        return t1[u % (LH + 1), y] + ry2[i], t2[u % (LH + 1), x] + rx2[i]

    def rs_steps(k, n, finish):
        @pl.when(jnp.logical_and(k >= LD, k < n + LD))
        def _():
            rs_stage2(k - LD)

        @pl.when(jnp.logical_and(k >= LD + LX, k < n + LD + LX))
        def _():
            rs_stage3(k - LD - LX)

        @pl.when(jnp.logical_and(k >= LT, k < n + LT))
        def _():
            finish(k - LT, *rs_stage4(k - LT))

    def rs_sends(k, n):
        @pl.when(jnp.logical_and(k >= 0, k < n))
        def _():
            rs_d(k).start()

        @pl.when(jnp.logical_and(k >= LD, k < n + LD))
        def _():
            rs_x(k - LD).start()
            rs_y(k - LD).start()

        @pl.when(jnp.logical_and(k >= LD + LX, k < n + LD + LX))
        def _():
            rs_x2(k - LD - LX).start()
            rs_y2(k - LD - LX).start()

    def m_send(b):
        return send(xbuf.at[b], mpeer.at[b], ms.at[b], mr.at[b], zp)

    def out_send(b):
        return send(mpeer.at[b, :, mine], xbuf.at[b, :, mine], os_.at[b], or_.at[b], zp)

    def hid_send(u):
        i = u % SLOTS
        return send(hown.at[u % (LH + 1)], hrecv.at[i], hs.at[i], hr.at[i], zp)

    for d in (z_q(0), z_k(0), z_v(0), z_oq(0)[0] if PAIRED[0] else z_o(0)):
        d.start()
    first = [pltpu.make_async_copy(x_ref, xbuf, wl.at[0])]
    for d in first:
        d.start()
    for d in first:
        d.wait()

    def first_rows(b, carry):
        hst[0] = _norm(xbuf[b], ga_ref[pl.ds(0, 1), :])
        d = h_store(ha.at[0], b, 0)
        d.start()
        d.wait()
        ag_send_own(ha.at[0], sa, ra, b)
        return carry

    lax.fori_loop(0, NB, first_rows, 0)
    if PAIRED[0]:
        w_send(0).start()
        for b in range(NB):
            for half in range(PAIR):
                res_send(b, half).start()

    def first_forward(i, carry):
        ag_fwd1(ha.at[0], sa, ra, i, cut_a(0))

        @pl.when(i >= 1)
        def _():
            ag_fwd2(ha.at[0], sa, ra, i - 1, cut_a(0))

        return carry

    for ref, buf, sign in ((cos_ref, cbuf, 1.0), (sin_ref, sbuf, -1.0)):
        tab = ref[...].T
        tmp[...] = jnp.concatenate([sign * tab, tab], axis=1).reshape(4, 2, T, HD)
        buf[0] = tmp[:, c]
        buf[1] = tmp[:, 1 - c]

    lax.fori_loop(0, NB, first_forward, 0)
    w_send(1).start()
    def pass_m(l, k):
        h = hb.at[l]
        cut = cut_b(l)
        wait_m = LM[l]

        def at(lag, run):
            b, ok = lookup(table(OTHER[l]), k - lag - LT)
            pl.when(ok)(lambda: run(b))

        def own(b):
            return PAIR * b + z

        def theirs(b):
            return PAIR * b + 1 - z

        def send_own(b):
            h_store(h, own(b), 0).wait()
            ag_send_own(h, sb, rb, own(b))

        def start_own(b):
            hst[0] = _norm(xbuf[b], gm_ref[pl.ds(l, 1), :])
            h_store(h, own(b), 0).start()
            m_send(b).start()

        def send_theirs(b):
            h_store(h, theirs(b), 1).wait()
            ag_send_own(h, sb, rb, theirs(b))

        def start_theirs(b):
            m_send(b).wait()
            hst[1] = _norm(mpeer[b], gm_ref[pl.ds(l, 1), :])
            h_store(h, theirs(b), 1).start()

        own_1, own_2, theirs_1, theirs_2 = LAGS_M[l]
        at(1, send_own)
        at(0, start_own)
        at(wait_m + 1, send_theirs)
        at(wait_m, start_theirs)
        at(own_1, lambda b: ag_fwd1(h, sb, rb, own(b), cut))
        at(theirs_1, lambda b: ag_fwd1(h, sb, rb, theirs(b), cut))
        at(own_2, lambda b: ag_fwd2(h, sb, rb, own(b), cut))
        at(theirs_2, lambda b: ag_fwd2(h, sb, rb, theirs(b), cut))

    def pass_y(l, s):
        last = l + 1 == n_layers
        free = FREE if last else 0

        @when(s >= free, s < NU, s % PAIR == 1 - z)
        def _():
            out_send(half_of(s)).start()

        if last:
            @pl.when(s == free)
            def _():
                for b in range(half_of(free)):
                    out_send(b).start()

        def at(lag, run):
            i = s - lag - 1
            when(within(i, NU), even(i))(lambda: run(half_of(i)))

        def got(b):
            out_send(b).wait()
            hst[0] = _norm(xbuf[b], ga_ref[pl.ds(l + 1, 1), :])
            h_store(ha.at[l + 1], b, 0).start()
            for half in range(PAIR):
                res_send(b, half).start()

        if not last:
            at(1, got)
            h, cut = ha.at[l + 1], cut_a(l + 1)

            def send_own(b):
                h_store(h, b, 0).wait()
                ag_send_own(h, sa, ra, b)

            at(2, send_own)
            at(LAGS_Y[0], lambda b: ag_fwd1(h, sa, ra, b, cut))
            at(LAGS_Y[1], lambda b: ag_fwd2(h, sa, ra, b, cut))

    def add(buf, b, start, low, high):
        for at, part in ((start, low), (start + V, high)):
            cols = lanes(at, V)
            buf[b, :, cols] = (buf[b, :, cols].astype(F32) + part).astype(BF16)

    def finish_y(s, low, high):
        b = half_of(s)
        pl.when(s % PAIR == z)(lambda: add(xbuf, b, z * W, low, high))
        pl.when(s % PAIR == 1 - z)(lambda: add(mpeer, b, z * W, low, high))

    def finish_m(u, low, high):
        half = z + (u // NB) * (1 - z - z)
        add(xbuf, u % NB, half * W, low, high)

    def a_steps(l):
        return len(ATTEND[l])

    def a_attend(l, k):
        return lookup(table(ATTEND[l]), k)

    def a_unit(l, k):
        own, oth = table(OWN[l]), table(OTHER[l])
        b_own, is_own = lookup(own, k)
        b_oth, is_oth = lookup(oth, k)
        u, _ = lookup({i: n for n, i in enumerate(sorted({**own, **oth}))}, k)
        return jnp.where(is_own, b_own, b_oth), u, is_own, is_oth

    def a_stages(l, k):
        if not PAIRED[l]:
            rs_steps(k, NU, finish_m)
            return

        def at(lag):
            b, u, own, oth = a_unit(l, k - lag)
            half = jnp.where(own, z, 1 - z)
            return b, u, half, jnp.logical_or(own, oth)

        _, u2, _, ok2 = at(LD)

        @pl.when(ok2)
        def _():
            ra_d(u2).wait()
            cols = low_v
            pown[u2 % SLOTS, :, :, :, cols] = pown[u2 % SLOTS, :, :, :, cols] + rd[u2 % PAIR, :, :, :, cols]

        b3, u3, half3, ok3 = at(LD + LX)

        @pl.when(ok3)
        def _():
            i = u3 % SLOTS
            ra_y(u3).wait()
            res_send(b3, half3).wait_recv()
            cols = lanes(half3 * W + x * V, V)
            xbuf[b3, :, cols] = (xbuf[b3, :, cols].astype(F32)
                                 + (pown[i, y, x, :, low_v] + ry[i, x])).astype(BF16)
            res = xres[b3, :, lanes(half3 * V, V)].astype(F32)
            mst[u3 % (LH + 1)] = (res + (pown[i, y, 1 - x, :, low_v] + ry[i, 1 - x])).astype(BF16)

        b4, u4, half4, ok4 = at(LT)
        pl.when(ok4)(lambda: ra_m(u4, b4, half4).wait())

    def a_sends(l, k):
        if not PAIRED[l]:
            rs_sends(k, NU)
            return

        def at(lag):
            b, u, own, oth = a_unit(l, k - lag)
            return b, u, jnp.where(own, z, 1 - z), jnp.logical_or(own, oth)

        _, u1, _, ok1 = at(0)
        pl.when(ok1)(lambda: ra_d(u1).start())
        _, u2, _, ok2 = at(LD)
        pl.when(ok2)(lambda: ra_y(u2).start())
        b3, u3, half3, ok3 = at(LD + LX)
        pl.when(ok3)(lambda: ra_m(u3, b3, half3).start())

    def b_steps(l):
        return GAP[l] + LH + NU + EXTRA[l]

    def pos_of(r):
        rail = r // (CHIPS * T)
        return CORES * T * ((r // T) % CHIPS) + T * ((c + rail) % CORES) + r % T

    def attend(l, b, h, wa_o, wa_r, o_all):
        ag_finish(h, sa, ra, b, cut_a(l))
        i = b % PAIR
        acc = jnp.dot(hv[i, :, :, :, mine].reshape(R, W), wa_o[...], preferred_element_type=F32)
        acc += jnp.dot(hv[i, :, :, :, other].reshape(R, W), wa_r[...], preferred_element_type=F32)
        qkv = acc.astype(BF16)
        cosv = cbuf[...].reshape(R, HD)
        sinv = sbuf[...].reshape(R, HD)

        def rope(t):
            t = t.astype(F32)
            return (t * cosv + pltpu.roll(t, HD // 2, 1) * sinv).astype(BF16)

        mask = pos_of(lax.broadcasted_iota(jnp.int32, (R, R), 0)) >= pos_of(
            lax.broadcasted_iota(jnp.int32, (R, R), 1))
        kk = rope(qkv[:, QW:QW + HD])
        vv = qkv[:, QW + HD:]
        for g in range(QW // HD):
            sc = lax.dot_general(rope(qkv[:, g * HD:(g + 1) * HD]), kk, NT, preferred_element_type=F32)
            sc = jnp.where(mask, sc * HD ** -0.5, -jnp.inf)
            e = jnp.exp(sc - jnp.max(sc, axis=-1, keepdims=True))
            p = (e / jnp.sum(e, axis=-1, keepdims=True)).astype(BF16)
            o_all[b, :, g * HD:(g + 1) * HD] = jnp.dot(p, vv, preferred_element_type=F32).astype(BF16)

    def loop_a(l, wa_o, wa_r, w_own, w_oth, o_all):
        h = ha.at[l]
        my_v = lanes(x * V, V)
        loads = [pltpu.make_async_copy(wq_ref.at[l], wa_o.at[:, pl.ds(0, QW)], wl.at[0]),
                 pltpu.make_async_copy(wk_ref.at[l], wa_o.at[:, pl.ds(QW, HD)], wl.at[1]),
                 pltpu.make_async_copy(wv_ref.at[l], wa_o.at[:, pl.ds(QW + HD, HD)], wl.at[2]),
                 pltpu.make_async_copy(wo_ref.at[l, :, my_v] if PAIRED[l] else wo_ref.at[l],
                                       w_own.at[0], wl.at[3])]
        from_x = pltpu.make_async_copy(rw.at[l], w_own.at[1], wl.at[7]) if PAIRED[l] else None
        if l > 0:
            loads.append(from_x)
        for d in loads:
            d.start()
        ag_load(h, sa, ra, 0)
        for d in (z_q(l), z_k(l), z_v(l)):
            d.wait()
        more = [pltpu.make_async_copy(rq.at[l], wa_r.at[:, pl.ds(0, QW)], wl.at[4]),
                pltpu.make_async_copy(rk.at[l], wa_r.at[:, pl.ds(QW, HD)], wl.at[5]),
                pltpu.make_async_copy(rv.at[l], wa_r.at[:, pl.ds(QW + HD, HD)], wl.at[6])]
        for d in more:
            d.start()
        for d in loads + more:
            d.wait()
        first_other = min(table(OTHER[l]))

        def step(k, carry):
            if l == 0:
                @pl.when(k == 0)
                def _():
                    ag_fwd2(h, sa, ra, NB - 1, cut_a(0))

            bn, next_ok = a_attend(l, k + 1)
            pl.when(next_ok)(lambda: ag_load(h, sa, ra, bn))
            ba, ok = a_attend(l, k)
            pl.when(ok)(lambda: attend(l, ba, h, wa_o, wa_r, o_all))
            b, u, own, oth = a_unit(l, k)

            if PAIRED[l] and l == 0:
                @pl.when(k == min(table(OWN[l])))
                def _():
                    w_send(l).wait()
                    z_oq(l)[1].start()
                    from_x.start()
                    from_x.wait()

            @pl.when(own)
            def _():
                if not PAIRED[l]:
                    store_product(u, [(o_all[b], w_own.at[0], None)], W)
                else:
                    o_send(o_all, b).wait()
                    store_product(u, [(o_all[b], w_own.at[0], None), (ox[b % (NB - 1)], w_own.at[1], None)], V)

            @pl.when(k == first_other)
            def _():
                got = z_oq(l) if PAIRED[l] else (z_o(l),)
                for d in got:
                    d.wait()
                if not PAIRED[l]:
                    into = [pltpu.make_async_copy(ro, w_oth.at[0], wl.at[5])]
                else:
                    into = [pltpu.make_async_copy(row.at[l, i], w_oth.at[i], wl.at[5 + i]) for i in range(2)]
                for d in into:
                    d.start()
                for d in into:
                    d.wait()

            @pl.when(oth)
            def _():
                if not PAIRED[l]:
                    store_product(u, [(o_all[b], w_oth.at[0], None)], W)
                else:
                    store_product(u, [(o_all[b], w_oth.at[0], None), (ox[b % (NB - 1)], w_oth.at[1], None)], V)

            if l > 0:
                rs_steps(NU + EXTRA[l - 1] + k, NU, finish_y)
            a_stages(l, k)
            if l > 0:
                rs_sends(NU + EXTRA[l - 1] + k, NU)
            if PAIRED[l]:
                @pl.when(ok)
                def _():
                    for half in range(2):
                        res_send(ba, half).wait_send()
                    o_send(o_all, ba).start()

            a_sends(l, k)
            if l > 0:
                pass_y(l - 1, NU + EXTRA[l - 1] + k - LT)
            pass_m(l, k)

            parts((O_IN_B[l - 1], O_IN_A[l]), k, functools.partial(z_o_part, l))
            parts((GU_IN_A[l],), k, functools.partial(z_gate_up_part, l))
            return carry

        lax.fori_loop(0, a_steps(l), step, 0)

    def loop_b(l, g_o, g_r, u_o, u_r, wd_v):
        h = hb.at[l]
        j0 = GAP[l]
        loads = [pltpu.make_async_copy(wg_ref.at[l, mine_h], g_o, wl.at[0]),
                 pltpu.make_async_copy(wu_ref.at[l, mine_h], u_o, wl.at[1]),
                 pltpu.make_async_copy(wd_ref.at[l], wd_v, wl.at[2])]
        more = [pltpu.make_async_copy(rg.at[l], g_r, wl.at[3]),
                pltpu.make_async_copy(ru.at[l], u_r, wl.at[4])]
        for d in loads:
            d.start()

        def step(k, carry):
            @pl.when(k == j0)
            def _():
                for d in (z_g(l), z_u(l)):
                    d.wait()
                for d in more:
                    d.start()
                for d in loads + more:
                    d.wait()

            @when(k >= j0 - 1, k < j0 + NU - 1)
            def _():
                ag_load(h, sb, rb, k - j0 + 1)

            @when(k >= j0, k < j0 + NU)
            def _():
                u = k - j0
                ag_finish(h, sb, rb, u, cut_b(l))
                i = u % PAIR
                hm = hv[i, :, :, :, mine].reshape(R, W)
                ho = hv[i, :, :, :, other].reshape(R, W)
                gate = lax.dot_general(g_o[...], hm, NT, preferred_element_type=F32)
                gate += lax.dot_general(g_r[...], ho, NT, preferred_element_type=F32)
                up = lax.dot_general(u_o[...], hm, NT, preferred_element_type=F32)
                up += lax.dot_general(u_r[...], ho, NT, preferred_element_type=F32)
                hown[u % (LH + 1)] = (jax.nn.silu(gate) * up).astype(BF16)

            v = k - j0 - LH

            @pl.when(within(v, NU))
            def _():
                hid_send(v).wait()
                store_product(v, [(hown[v % (LH + 1)], wd_v, mine_h), (hrecv[v % SLOTS], wd_v, theirs_h)], W)

            a_stages(l, a_steps(l) + k)
            rs_steps(v, NU, finish_y)

            @when(k >= j0, k < j0 + NU)
            def _():
                hid_send(k - j0).start()

            a_sends(l, a_steps(l) + k)
            rs_sends(v, NU)
            pass_m(l, a_steps(l) + k)
            pass_y(l, v - LT)

            parts((GU_IN_A[l], GU_IN_B[l]), k, functools.partial(z_gate_up_part, l))
            if l + 1 < n_layers:
                @pl.when(k == min(table(O_IN_B[l].replace("0", "-"))))
                def _():
                    w_send(l + 1).wait()

                parts((QKV_IN_B[l],), k, functools.partial(z_qkv_part, l + 1))
                parts((O_IN_B[l],), k, functools.partial(z_o_part, l + 1))

            return carry

        lax.fori_loop(0, b_steps(l), step, 0)

    for l in range(n_layers):
        pl.run_scoped(
            functools.partial(loop_a, l),
            pltpu.VMEM((W, QW + 2 * HD), BF16), pltpu.VMEM((W, QW + 2 * HD), BF16),
            pltpu.VMEM((2, QW, V) if PAIRED[l] else (1, QW, W), BF16),
            pltpu.VMEM((2, QW, V) if PAIRED[l] else (1, QW, W), BF16), pltpu.VMEM((NB, R, QW), BF16))
        pl.run_scoped(
            functools.partial(loop_b, l),
            pltpu.VMEM((HB, W), BF16), pltpu.VMEM((HB, W), BF16),
            pltpu.VMEM((HB, W), BF16), pltpu.VMEM((HB, W), BF16), pltpu.VMEM((2 * HB, W), BF16))

    def tail(v, carry):
        rs_steps(v, NU, finish_y)
        rs_sends(v, NU)
        pass_y(n_layers - 1, v - LT)
        return carry

    lax.fori_loop(NU, NU + LT + 2, tail, 0)
    for b in range(NB):
        out_send(b).wait()
        y_store(b).start()
    for b in range(NB):
        y_store(b).wait()


def solution(mesh):
    act_spec = P("fsdp", "model", None)
    col_spec = P(None, "fsdp", "model")
    row_spec = P(None, "model", "fsdp")

    def device_step(x_in, gain_attn, gain_mlp, rope_cos, rope_sin, w_q, w_k, w_v, w_o, w_gate, w_up, w_down):
        L, NB, T, D = w_q.shape[0], *x_in.shape
        W, V = D // PAIR, D // CHIPS
        HB = w_gate.shape[-1] // PAIR
        NU, R = PAIR * NB, CHIPS * CORES * T
        HD = PAIR * rope_cos.shape[-1]
        QW = w_o.shape[1]
        hbm = pl.BlockSpec(memory_space=pl.ANY)
        vmem = pl.BlockSpec(memory_space=pltpu.VMEM)
        sds = jax.ShapeDtypeStruct

        def buf(dtype, *shape):
            return pltpu.VMEM(shape, dtype)

        def sems(*shape):
            return pltpu.SemaphoreType.DMA(shape)

        args = (x_in, gain_attn, gain_mlp, rope_cos.T, rope_sin.T, w_q, w_k, w_v, w_o,
                jnp.swapaxes(w_gate, 1, -1), jnp.swapaxes(w_up, 1, -1), w_down)
        half_rows, plane_rows = (L, HB, W), (CORES, CHIPS, T, D)
        shapes = [x_in.shape, w_q.shape, w_k.shape, w_v.shape, w_o.shape[1:], half_rows, half_rows,
                  (L, NB) + plane_rows, (L, NU) + plane_rows, (L, QW, V), (L, PAIR, QW, V)]
        unit, hop = (PAIR, PAIR, T, W), (PAIR, T, V)
        in_flight, hidden, tables = LH + 1, (HB, R), (CORES, CHIPS, T, HD)
        outs = pl.pallas_call(
            _kernel,
            name="two_layers",
            in_specs=[vmem if a.ndim <= PAIR else hbm for a in args],
            out_specs=[hbm] * len(shapes),
            out_shape=[sds(shape, BF16) for shape in shapes],
            scratch_shapes=[
                buf(BF16, NB, T, D), buf(BF16, NB, T, D), buf(BF16, PAIR, T, D), buf(BF16, PAIR, *plane_rows),
                buf(F32, SLOTS, *unit), buf(F32, PAIR, *unit), buf(F32, PAIR, *unit),
                buf(F32, in_flight, *hop), buf(F32, in_flight, *hop), buf(F32, SLOTS, *hop), buf(F32, SLOTS, *hop),
                buf(F32, SLOTS, T, V), buf(F32, SLOTS, T, V), buf(BF16, in_flight, *hidden), buf(BF16, SLOTS, *hidden),
                buf(F32, *tables), buf(F32, *tables), buf(F32, CHIPS, CORES, T, HD),
                buf(BF16, NB - 1, R, QW), buf(BF16, NB, T, W), buf(BF16, in_flight, T, V)]
            + [sems(int(ch)) for ch in SEMS] + [sems(NB, CHIPS + 1), sems(NB, CHIPS + 1), sems(NU, CHIPS + 1),
                                                sems(NU, CHIPS + 1), sems(NB, PAIR), sems(NB, PAIR),
                                                sems(L, PAIR + 1), sems(L, PAIR + 1)],
            compiler_params=pltpu.CompilerParams(
                collective_id=0, has_side_effects=True, vmem_limit_bytes=67_000_000),
        )(*args)
        return outs[0]

    return jax.shard_map(
        device_step, mesh=mesh,
        in_specs=(act_spec, P(), P(), P(), P(), col_spec, col_spec, col_spec, row_spec, col_spec, col_spec, row_spec),
        out_specs=act_spec, check_vma=False)
```

```python
import functools

import jax
import jax.numpy as jnp
from jax import lax
from jax.experimental import pallas as pl
from jax.experimental.pallas import tpu as pltpu
from jax.sharding import PartitionSpec as P

EPS = 1e-5
MESH = pl.DeviceIdType.MESH
NN = (((1,), (0,)), ((), ()))
NT = (((1,), (1,)), ((), ()))
TN = (((0,), (0,)), ((), ()))
LD = 1
LX = 2
LT = LD + 2 * LX
LH = 2
LM = (7, 4)
LAGS_M = ((10, 13, 10, 12), (6, 10, 7, 14))
LAGS_Y = (4, 7)
FREE = 6
EXTRA = (7, 0)
PAIRED = (False, True)
GAP = (12, 8)
SLOTS, CHIPS, CORES, PAIR = 4, 4, 2, 2
ALIGN, LANES = 16, 128
SEMS = "4422224444444488884444" + "22888"
GU, ATTN = 18, 8

CUT_A = (29, 34)
CUT_B = (20, 19)
CUTS = 40

ATTEND = ("01234567--------", "0123-4-5--6---7---------------")
OWN = ("01234567--------", "---01234--5--6--7-------------")
OTHER = ("--------01234567", "---------0--1--2----3---456--7")
GU_IN_A = ("2000212321221211", "210002120011200220002023221010")
GU_IN_B = ("0132101231", "232")
QKV_IN_B = ("0000000000010100000001000100012010000", "")
O_IN_A = ("", "000011")
O_IN_B = ("0000000000000000000000100000110000201", "")
F32 = jnp.float32
BF16 = jnp.bfloat16


def _norm(rows, gain):
    rows = rows.astype(F32)
    mean_sq = jnp.mean(rows * rows, axis=-1, keepdims=True)
    return (rows * lax.rsqrt(mean_sq + EPS) * gain).astype(BF16)


def _kernel(
    x_ref, ga_ref, gm_ref, cos_ref, sin_ref, wq_ref, wk_ref, wv_ref, wo_ref, wg_ref, wu_ref, wd_ref,
    y_ref, rq, rk, rv, ro, rg, ru, ha, hb, rw, row,
    xbuf, mpeer, hst, hv, pown, psib, rd, t1, t2, rx, ry, rx2, ry2, hown, hrecv, cbuf, sbuf, tmp, ox, xres, mst,
    zs, zr, gs, gr, ds, dr, xs, xr, ys, yr, x2s, x2r, y2s, y2r, ms, mr, os_, or_, hs, hr, mxs, mxr,
    loc, hvs, wl, oxs, oxr, sa, ra, sb, rb, xrs, xrr, wxs, wxr,
):
    n_layers = wq_ref.shape[0]
    NB, T, D = x_ref.shape
    W, V = D // PAIR, D // CHIPS
    QW = wq_ref.shape[2]
    HD = wk_ref.shape[2]
    HB = wg_ref.shape[1] // PAIR
    R = CHIPS * CORES * T
    NU = PAIR * NB

    z = lax.axis_index("fsdp")
    m = lax.axis_index("model")
    y, x, c, q = m // 4, (m // 2) % 2, m % 2, m // 2
    qx, qy, qd = q + 1 - 2 * x, q + 2 - 4 * y, 3 - q
    zp, xp, yp, sp = (1 - z, m), (z, m + 2 - 4 * x), (z, m + 4 - 8 * y), (z, m + 1 - 2 * c)

    def lanes(start, size):
        return pl.ds(pl.multiple_of(start, LANES), size)

    def rows(start, size):
        return pl.ds(pl.multiple_of(start, ALIGN), size)

    mine, other = lanes(z * W, W), lanes((1 - z) * W, W)
    low_v, high_v = pl.ds(0, V), pl.ds(V, V)

    def even(i):
        return i % PAIR == 0

    def half_of(i):
        return i // PAIR

    def when(*conds):
        return pl.when(functools.reduce(jnp.logical_and, conds))

    def within(k, n):
        return jnp.logical_and(k >= 0, k < n)

    def lookup(table, k):
        runs = []
        for i in sorted(table):
            if runs:
                run = runs[-1]
                stride = i - run[-1]
                if table[i] == table[run[-1]] + 1 and stride in (1, PAIR) and (
                        len(run) == 1 or stride == run[-1] - run[-2]):
                    run.append(i)
                    continue
            runs.append([i])
        value, there = None, None
        for run in reversed(runs):
            first, last = run[0], run[-1]
            stride = run[1] - first if len(run) > 1 else 1
            ok = jnp.logical_and(k >= first, k <= last)
            if stride > 1:
                ok = jnp.logical_and(ok, (k - first) % stride == 0)
            val = (k - first) // stride + table[first]
            value = val if value is None else jnp.where(k <= last, val, value)
            there = ok if there is None else jnp.logical_or(there, ok)
        return value, there

    def table(text):
        return {i: int(ch) for i, ch in enumerate(text) if ch.isdigit()}

    def parts(texts, k, start):
        done = sum(int(ch) for text in texts[:-1] for ch in text)
        for i, ch in enumerate(texts[-1]):
            n = int(ch)
            if n:
                @pl.when(k == i)
                def _():
                    for j in range(done, done + n):
                        start(j)
            done += n

    barrier = pltpu.get_barrier_semaphore()
    for dev in (zp, xp, yp, sp):
        pl.semaphore_signal(barrier, inc=1, device_id=dev, device_id_type=MESH)
    pl.semaphore_wait(barrier, 4)

    def send(src, dst, s, r, dev):
        return pltpu.make_async_remote_copy(
            src_ref=src, dst_ref=dst, send_sem=s, recv_sem=r, device_id=dev, device_id_type=MESH)

    def z_q(l):
        return send(wq_ref.at[l], rq.at[l], zs.at[0], zr.at[0], zp)

    def z_k(l):
        return send(wk_ref.at[l], rk.at[l], zs.at[1], zr.at[1], zp)

    def z_v(l):
        return send(wv_ref.at[l], rv.at[l], zs.at[2], zr.at[2], zp)

    def z_o(l):
        return send(wo_ref.at[l], ro, zs.at[3], zr.at[3], zp)

    mine_h, theirs_h = rows(z * HB, HB), rows((1 - z) * HB, HB)

    def z_g(l):
        return send(wg_ref.at[l, theirs_h], rg.at[l], gs.at[0], gr.at[0], zp)

    def z_u(l):
        return send(wu_ref.at[l, theirs_h], ru.at[l], gs.at[1], gr.at[1], zp)

    def z_gate_up_part(l, j):
        size = HB // GU
        ref, out, i = (wg_ref, rg, 0) if j < GU else (wu_ref, ru, 1)
        at = (j % GU) * size
        send(ref.at[l, rows((1 - z) * HB + at, size)], out.at[l, pl.ds(at, size)], gs.at[i], gr.at[i], zp).start()

    def z_qkv_part(l, j):
        size = W // ATTN
        at = pl.ds(j * size, size)
        for i, (ref, out) in enumerate(((wq_ref, rq), (wk_ref, rk), (wv_ref, rv))):
            send(ref.at[l, at], out.at[l, at], zs.at[i], zr.at[i], zp).start()

    def z_o_part(l, j):
        size = QW // ATTN
        for d in z_oq(l, pl.ds(j * size, size)):
            d.start()

    def cut_of(share):
        return max(1, D // LANES * share // CUTS) * LANES

    def cut_a(l):
        return cut_of(CUT_A[l])

    def cut_b(l):
        return cut_of(CUT_B[l])

    def ag_own(h, s, r, u):
        own = h.at[u, 0, q]
        return [send(own, own, s.at[u, i], r.at[u, i], dev) for i, dev in enumerate((xp, yp))]

    def ag_fwd(h, s, r, u, cut):
        from_x, from_y = h.at[u, 0, qx, :, pl.ds(0, cut)], h.at[u, 0, qy, :, pl.ds(cut, D - cut)]
        return [send(from_x, from_x, s.at[u, 2], r.at[u, 2], yp), send(from_y, from_y, s.at[u, 3], r.at[u, 3], xp)]

    def ag_sib(h, s, r, u):
        return send(h.at[u, 0], h.at[u, 1], s.at[u, CHIPS], r.at[u, CHIPS], sp)

    def ag_send_own(h, s, r, u):
        for d in ag_own(h, s, r, u):
            d.start()

    def ag_fwd1(h, s, r, u, cut):
        for own, fwd in zip(ag_own(h, s, r, u), ag_fwd(h, s, r, u, cut)):
            own.wait_recv()
            fwd.start()

    def ag_fwd2(h, s, r, u, cut):
        for fwd in ag_fwd(h, s, r, u, cut):
            fwd.wait_recv()
        ag_sib(h, s, r, u).start()

    def ag_local(h, u):
        return pltpu.make_async_copy(h.at[u], hv.at[u % PAIR], hvs.at[u % PAIR])

    def ag_load(h, s, r, u):
        ag_sib(h, s, r, u).wait_recv()
        ag_local(h, u).start()

    def ag_finish(h, s, r, u, cut):
        ag_local(h, u).wait()
        for d in ag_own(h, s, r, u) + ag_fwd(h, s, r, u, cut) + [ag_sib(h, s, r, u)]:
            d.wait_send()

    def y_store(b):
        return pltpu.make_async_copy(xbuf.at[b], y_ref.at[b], oxs.at[b])

    def h_store(h, u, j):
        return pltpu.make_async_copy(hst.at[j], h.at[u, 0, q], loc.at[j])

    def rs_d(u):
        return send(psib.at[u % PAIR], rd.at[u % PAIR], ds.at[u % PAIR], dr.at[u % PAIR], sp)

    def rs_x(u):
        i = u % SLOTS
        return send(pown.at[i, :, 1 - x, :, low_v], rx.at[i], xs.at[i], xr.at[i], xp)

    def rs_y(u):
        i = u % SLOTS
        return send(pown.at[i, 1 - y, :, :, high_v], ry.at[i], ys.at[i], yr.at[i], yp)

    def ra_d(u):
        return send(psib.at[u % PAIR, :, :, :, low_v], rd.at[u % PAIR, :, :, :, low_v],
                    ds.at[u % PAIR], dr.at[u % PAIR], sp)

    def ra_y(u):
        i = u % SLOTS
        return send(pown.at[i, 1 - y, :, :, low_v], ry.at[i], ys.at[i], yr.at[i], yp)

    def ra_m(u, b, half):
        cols = lanes(half * W + x * V, V)
        return send(mst.at[u % (LH + 1)], xbuf.at[b, :, cols], mxs.at[u % SLOTS], mxr.at[u % SLOTS], xp)

    def o_send(o_all, b):
        return send(o_all.at[b], ox.at[b % (NB - 1)], oxs.at[b], oxr.at[b], xp)

    def res_send(b, half):
        src = lanes(half * W + (1 - x) * V, V)
        dst = lanes(half * V, V)
        return send(xbuf.at[b, :, src], xres.at[b, :, dst], xrs.at[b, half], xrr.at[b, half], xp)

    def w_send(l):
        cols = lanes((1 - x) * V, V)
        return send(wo_ref.at[l, :, cols], rw.at[l], wxs.at[l, 0], wxr.at[l, 0], xp)

    def z_oq(l, rows=slice(None)):
        cols = lanes(x * V, V)
        return (send(wo_ref.at[l, rows, cols], row.at[l, 0, rows], wxs.at[l, 1], wxr.at[l, 1], zp),
                send(rw.at[l, rows], row.at[l, 1, rows], wxs.at[l, 2], wxr.at[l, 2], zp))

    def rs_x2(u):
        i = u % SLOTS
        return send(t2.at[u % (LH + 1), 1 - x], rx2.at[i], x2s.at[i], x2r.at[i], xp)

    def rs_y2(u):
        i = u % SLOTS
        return send(t1.at[u % (LH + 1), 1 - y], ry2.at[i], y2s.at[i], y2r.at[i], yp)

    def store_product(u, pairs, width):
        half = W // 2
        for j in range(width // half):
            cols = pl.ds(j * half, half)
            acc = None
            for a, w, rows in pairs:
                wv_ = w[:, cols] if rows is None else w[rows, cols]
                p = lax.dot_general(a, wv_, TN if rows is not None else NN, preferred_element_type=F32)
                acc = p if acc is None else acc + p
            pown[u % SLOTS, :, :, :, cols] = acc[: R // 2].reshape(2, 2, T, half)
            psib[u % PAIR, :, :, :, cols] = acc[R // 2:].reshape(2, 2, T, half)

    def rs_stage2(u):
        rs_d(u).wait()
        pown[u % SLOTS] = pown[u % SLOTS] + rd[u % PAIR]

    def rs_stage3(u):
        i = u % SLOTS
        rs_x(u).wait()
        rs_y(u).wait()
        t1[u % (LH + 1)] = pown[i, :, x, :, low_v] + rx[i]
        t2[u % (LH + 1)] = pown[i, y, :, :, high_v] + ry[i]

    def rs_stage4(u):
        i = u % SLOTS
        rs_x2(u).wait()
        rs_y2(u).wait()
        return t1[u % (LH + 1), y] + ry2[i], t2[u % (LH + 1), x] + rx2[i]

    def rs_steps(k, n, finish):
        @pl.when(jnp.logical_and(k >= LD, k < n + LD))
        def _():
            rs_stage2(k - LD)

        @pl.when(jnp.logical_and(k >= LD + LX, k < n + LD + LX))
        def _():
            rs_stage3(k - LD - LX)

        @pl.when(jnp.logical_and(k >= LT, k < n + LT))
        def _():
            finish(k - LT, *rs_stage4(k - LT))

    def rs_first(k, n):
        pl.when(within(k, n))(lambda: rs_d(k).start())

    def rs_sends(k, n):
        @pl.when(jnp.logical_and(k >= LD, k < n + LD))
        def _():
            rs_x(k - LD).start()
            rs_y(k - LD).start()

        @pl.when(jnp.logical_and(k >= LD + LX, k < n + LD + LX))
        def _():
            rs_x2(k - LD - LX).start()
            rs_y2(k - LD - LX).start()

    def m_send(b):
        return send(xbuf.at[b], mpeer.at[b], ms.at[b], mr.at[b], zp)

    def out_send(b):
        return send(mpeer.at[b, :, mine], xbuf.at[b, :, mine], os_.at[b], or_.at[b], zp)

    def hid_send(u):
        i = u % SLOTS
        return send(hown.at[u % (LH + 1)], hrecv.at[i], hs.at[i], hr.at[i], zp)

    for d in (z_q(0), z_k(0), z_v(0), z_oq(0)[0] if PAIRED[0] else z_o(0)):
        d.start()
    first = [pltpu.make_async_copy(x_ref, xbuf, wl.at[0])]
    for d in first:
        d.start()
    for d in first:
        d.wait()

    def first_rows(b, carry):
        hst[0] = _norm(xbuf[b], ga_ref[pl.ds(0, 1), :])
        d = h_store(ha.at[0], b, 0)
        d.start()
        d.wait()
        ag_send_own(ha.at[0], sa, ra, b)
        return carry

    lax.fori_loop(0, NB, first_rows, 0)
    if PAIRED[0]:
        w_send(0).start()
        for b in range(NB):
            for half in range(PAIR):
                res_send(b, half).start()

    def first_forward(i, carry):
        ag_fwd1(ha.at[0], sa, ra, i, cut_a(0))

        @pl.when(i >= 1)
        def _():
            ag_fwd2(ha.at[0], sa, ra, i - 1, cut_a(0))

        return carry

    for ref, buf, sign in ((cos_ref, cbuf, 1.0), (sin_ref, sbuf, -1.0)):
        tab = ref[...].T
        tmp[...] = jnp.concatenate([sign * tab, tab], axis=1).reshape(4, 2, T, HD)
        buf[0] = tmp[:, c]
        buf[1] = tmp[:, 1 - c]

    lax.fori_loop(0, NB, first_forward, 0)
    w_send(1).start()
    def pass_m(l, k):
        h = hb.at[l]
        cut = cut_b(l)
        wait_m = LM[l]

        def at(lag, run):
            b, ok = lookup(table(OTHER[l]), k - lag - LT)
            pl.when(ok)(lambda: run(b))

        def own(b):
            return PAIR * b + z

        def theirs(b):
            return PAIR * b + 1 - z

        def send_own(b):
            h_store(h, own(b), 0).wait()
            ag_send_own(h, sb, rb, own(b))

        def start_own(b):
            hst[0] = _norm(xbuf[b], gm_ref[pl.ds(l, 1), :])
            h_store(h, own(b), 0).start()
            m_send(b).start()

        def send_theirs(b):
            h_store(h, theirs(b), 1).wait()
            ag_send_own(h, sb, rb, theirs(b))

        def start_theirs(b):
            m_send(b).wait()
            hst[1] = _norm(mpeer[b], gm_ref[pl.ds(l, 1), :])
            h_store(h, theirs(b), 1).start()

        own_1, own_2, theirs_1, theirs_2 = LAGS_M[l]
        at(1, send_own)
        at(0, start_own)
        at(wait_m + 1, send_theirs)
        at(wait_m, start_theirs)
        at(own_1, lambda b: ag_fwd1(h, sb, rb, own(b), cut))
        at(theirs_1, lambda b: ag_fwd1(h, sb, rb, theirs(b), cut))
        at(own_2, lambda b: ag_fwd2(h, sb, rb, own(b), cut))
        at(theirs_2, lambda b: ag_fwd2(h, sb, rb, theirs(b), cut))

    def pass_y(l, s):
        last = l + 1 == n_layers
        free = FREE if last else 0

        @when(s >= free, s < NU, s % PAIR == 1 - z)
        def _():
            out_send(half_of(s)).start()

        if last:
            @pl.when(s == free)
            def _():
                for b in range(half_of(free)):
                    out_send(b).start()

        def at(lag, run):
            i = s - lag - 1
            when(within(i, NU), even(i))(lambda: run(half_of(i)))

        def got(b):
            out_send(b).wait()
            hst[0] = _norm(xbuf[b], ga_ref[pl.ds(l + 1, 1), :])
            h_store(ha.at[l + 1], b, 0).start()
            for half in range(PAIR):
                res_send(b, half).start()

        if not last:
            at(1, got)
            h, cut = ha.at[l + 1], cut_a(l + 1)

            def send_own(b):
                h_store(h, b, 0).wait()
                ag_send_own(h, sa, ra, b)

            at(2, send_own)
            at(LAGS_Y[0], lambda b: ag_fwd1(h, sa, ra, b, cut))
            at(LAGS_Y[1], lambda b: ag_fwd2(h, sa, ra, b, cut))

    def add(buf, b, start, low, high):
        for at, part in ((start, low), (start + V, high)):
            cols = lanes(at, V)
            buf[b, :, cols] = (buf[b, :, cols].astype(F32) + part).astype(BF16)

    def finish_y(s, low, high):
        b = half_of(s)
        pl.when(s % PAIR == z)(lambda: add(xbuf, b, z * W, low, high))
        pl.when(s % PAIR == 1 - z)(lambda: add(mpeer, b, z * W, low, high))

    def finish_m(u, low, high):
        half = z + (u // NB) * (1 - z - z)
        add(xbuf, u % NB, half * W, low, high)

    def a_steps(l):
        return len(ATTEND[l])

    def a_attend(l, k):
        return lookup(table(ATTEND[l]), k)

    def a_unit(l, k):
        own, oth = table(OWN[l]), table(OTHER[l])
        b_own, is_own = lookup(own, k)
        b_oth, is_oth = lookup(oth, k)
        u, _ = lookup({i: n for n, i in enumerate(sorted({**own, **oth}))}, k)
        return jnp.where(is_own, b_own, b_oth), u, is_own, is_oth

    def a_stages(l, k):
        if not PAIRED[l]:
            rs_steps(k, NU, finish_m)
            return

        def at(lag):
            b, u, own, oth = a_unit(l, k - lag)
            half = jnp.where(own, z, 1 - z)
            return b, u, half, jnp.logical_or(own, oth)

        _, u2, _, ok2 = at(LD)

        @pl.when(ok2)
        def _():
            ra_d(u2).wait()
            cols = low_v
            pown[u2 % SLOTS, :, :, :, cols] = pown[u2 % SLOTS, :, :, :, cols] + rd[u2 % PAIR, :, :, :, cols]

        b3, u3, half3, ok3 = at(LD + LX)

        @pl.when(ok3)
        def _():
            i = u3 % SLOTS
            ra_y(u3).wait()
            res_send(b3, half3).wait_recv()
            cols = lanes(half3 * W + x * V, V)
            xbuf[b3, :, cols] = (xbuf[b3, :, cols].astype(F32)
                                 + (pown[i, y, x, :, low_v] + ry[i, x])).astype(BF16)
            res = xres[b3, :, lanes(half3 * V, V)].astype(F32)
            mst[u3 % (LH + 1)] = (res + (pown[i, y, 1 - x, :, low_v] + ry[i, 1 - x])).astype(BF16)

        b4, u4, half4, ok4 = at(LT)
        pl.when(ok4)(lambda: ra_m(u4, b4, half4).wait())

    def a_first(l, k):
        _, u, own, oth = a_unit(l, k)
        first = ra_d if PAIRED[l] else rs_d
        pl.when(jnp.logical_or(own, oth))(lambda: first(u).start())

    def a_sends(l, k):
        if not PAIRED[l]:
            rs_sends(k, NU)
            return

        def at(lag):
            b, u, own, oth = a_unit(l, k - lag)
            return b, u, jnp.where(own, z, 1 - z), jnp.logical_or(own, oth)

        _, u2, _, ok2 = at(LD)
        pl.when(ok2)(lambda: ra_y(u2).start())
        b3, u3, half3, ok3 = at(LD + LX)
        pl.when(ok3)(lambda: ra_m(u3, b3, half3).start())

    def b_steps(l):
        return GAP[l] + LH + NU + EXTRA[l]

    def pos_of(r):
        rail = r // (CHIPS * T)
        return CORES * T * ((r // T) % CHIPS) + T * ((c + rail) % CORES) + r % T

    def attend(l, b, h, wa_o, wa_r, o_all):
        ag_finish(h, sa, ra, b, cut_a(l))
        i = b % PAIR
        acc = jnp.dot(hv[i, :, :, :, mine].reshape(R, W), wa_o[...], preferred_element_type=F32)
        acc += jnp.dot(hv[i, :, :, :, other].reshape(R, W), wa_r[...], preferred_element_type=F32)
        qkv = acc.astype(BF16)
        cosv = cbuf[...].reshape(R, HD)
        sinv = sbuf[...].reshape(R, HD)

        def rope(t):
            t = t.astype(F32)
            return (t * cosv + pltpu.roll(t, HD // 2, 1) * sinv).astype(BF16)

        mask = pos_of(lax.broadcasted_iota(jnp.int32, (R, R), 0)) >= pos_of(
            lax.broadcasted_iota(jnp.int32, (R, R), 1))
        kk = rope(qkv[:, QW:QW + HD])
        vv = qkv[:, QW + HD:]
        for g in range(QW // HD):
            sc = lax.dot_general(rope(qkv[:, g * HD:(g + 1) * HD]), kk, NT, preferred_element_type=F32)
            sc = jnp.where(mask, sc * HD ** -0.5, -jnp.inf)
            e = jnp.exp(sc - jnp.max(sc, axis=-1, keepdims=True))
            p = (e / jnp.sum(e, axis=-1, keepdims=True)).astype(BF16)
            o_all[b, :, g * HD:(g + 1) * HD] = jnp.dot(p, vv, preferred_element_type=F32).astype(BF16)

    def loop_a(l, wa_o, wa_r, w_own, w_oth, o_all):
        h = ha.at[l]
        my_v = lanes(x * V, V)
        loads = [pltpu.make_async_copy(wq_ref.at[l], wa_o.at[:, pl.ds(0, QW)], wl.at[0]),
                 pltpu.make_async_copy(wk_ref.at[l], wa_o.at[:, pl.ds(QW, HD)], wl.at[1]),
                 pltpu.make_async_copy(wv_ref.at[l], wa_o.at[:, pl.ds(QW + HD, HD)], wl.at[2]),
                 pltpu.make_async_copy(wo_ref.at[l, :, my_v] if PAIRED[l] else wo_ref.at[l],
                                       w_own.at[0], wl.at[3])]
        from_x = pltpu.make_async_copy(rw.at[l], w_own.at[1], wl.at[7]) if PAIRED[l] else None
        if l > 0:
            loads.append(from_x)
        for d in loads:
            d.start()
        ag_load(h, sa, ra, 0)
        for d in (z_q(l), z_k(l), z_v(l)):
            d.wait()
        more = [pltpu.make_async_copy(rq.at[l], wa_r.at[:, pl.ds(0, QW)], wl.at[4]),
                pltpu.make_async_copy(rk.at[l], wa_r.at[:, pl.ds(QW, HD)], wl.at[5]),
                pltpu.make_async_copy(rv.at[l], wa_r.at[:, pl.ds(QW + HD, HD)], wl.at[6])]
        for d in more:
            d.start()
        for d in loads + more:
            d.wait()
        first_other = min(table(OTHER[l]))

        def step(k, carry):
            if l == 0:
                @pl.when(k == 0)
                def _():
                    ag_fwd2(h, sa, ra, NB - 1, cut_a(0))

            bn, next_ok = a_attend(l, k + 1)
            pl.when(next_ok)(lambda: ag_load(h, sa, ra, bn))
            ba, ok = a_attend(l, k)
            pl.when(ok)(lambda: attend(l, ba, h, wa_o, wa_r, o_all))
            if l > 0:
                rs_steps(NU + EXTRA[l - 1] + k, NU, finish_y)
            a_stages(l, k)
            if l > 0:
                rs_sends(NU + EXTRA[l - 1] + k, NU)
            if PAIRED[l]:
                @pl.when(ok)
                def _():
                    for half in range(2):
                        res_send(ba, half).wait_send()
                    o_send(o_all, ba).start()

            a_sends(l, k)
            b, u, own, oth = a_unit(l, k)

            if PAIRED[l] and l == 0:
                @pl.when(k == min(table(OWN[l])))
                def _():
                    w_send(l).wait()
                    z_oq(l)[1].start()
                    from_x.start()
                    from_x.wait()

            @pl.when(own)
            def _():
                if not PAIRED[l]:
                    store_product(u, [(o_all[b], w_own.at[0], None)], W)
                else:
                    o_send(o_all, b).wait()
                    store_product(u, [(o_all[b], w_own.at[0], None), (ox[b % (NB - 1)], w_own.at[1], None)], V)

            @pl.when(k == first_other)
            def _():
                got = z_oq(l) if PAIRED[l] else (z_o(l),)
                for d in got:
                    d.wait()
                if not PAIRED[l]:
                    into = [pltpu.make_async_copy(ro, w_oth.at[0], wl.at[5])]
                else:
                    into = [pltpu.make_async_copy(row.at[l, i], w_oth.at[i], wl.at[5 + i]) for i in range(2)]
                for d in into:
                    d.start()
                for d in into:
                    d.wait()

            @pl.when(oth)
            def _():
                if not PAIRED[l]:
                    store_product(u, [(o_all[b], w_oth.at[0], None)], W)
                else:
                    store_product(u, [(o_all[b], w_oth.at[0], None), (ox[b % (NB - 1)], w_oth.at[1], None)], V)

            a_first(l, k)
            if l > 0:
                pass_y(l - 1, NU + EXTRA[l - 1] + k - LT)
            pass_m(l, k)

            parts((O_IN_B[l - 1], O_IN_A[l]), k, functools.partial(z_o_part, l))
            parts((GU_IN_A[l],), k, functools.partial(z_gate_up_part, l))
            return carry

        lax.fori_loop(0, a_steps(l), step, 0)

    def loop_b(l, g_o, g_r, u_o, u_r, wd_v):
        h = hb.at[l]
        j0 = GAP[l]
        loads = [pltpu.make_async_copy(wg_ref.at[l, mine_h], g_o, wl.at[0]),
                 pltpu.make_async_copy(wu_ref.at[l, mine_h], u_o, wl.at[1]),
                 pltpu.make_async_copy(wd_ref.at[l], wd_v, wl.at[2])]
        more = [pltpu.make_async_copy(rg.at[l], g_r, wl.at[3]),
                pltpu.make_async_copy(ru.at[l], u_r, wl.at[4])]
        for d in loads:
            d.start()

        def step(k, carry):
            @pl.when(k == j0 - 1)
            def _():
                z_g(l).wait()
                more[0].start()
                for d in loads:
                    d.wait()
                more[0].wait()

            @pl.when(k == j0)
            def _():
                z_u(l).wait()
                more[1].start()
                more[1].wait()

            @when(k >= j0 - 1, k < j0 + NU - 1)
            def _():
                ag_load(h, sb, rb, k - j0 + 1)

            @when(k >= j0, k < j0 + NU)
            def _():
                u = k - j0
                ag_finish(h, sb, rb, u, cut_b(l))
                i = u % PAIR
                hm = hv[i, :, :, :, mine].reshape(R, W)
                ho = hv[i, :, :, :, other].reshape(R, W)
                gate = lax.dot_general(g_o[...], hm, NT, preferred_element_type=F32)
                gate += lax.dot_general(g_r[...], ho, NT, preferred_element_type=F32)
                up = lax.dot_general(u_o[...], hm, NT, preferred_element_type=F32)
                up += lax.dot_general(u_r[...], ho, NT, preferred_element_type=F32)
                hown[u % (LH + 1)] = (jax.nn.silu(gate) * up).astype(BF16)

            v = k - j0 - LH
            a_stages(l, a_steps(l) + k)
            rs_steps(v, NU, finish_y)

            a_sends(l, a_steps(l) + k)
            rs_sends(v, NU)

            @pl.when(within(v, NU))
            def _():
                hid_send(v).wait()
                store_product(v, [(hown[v % (LH + 1)], wd_v, mine_h), (hrecv[v % SLOTS], wd_v, theirs_h)], W)

            @when(k >= j0, k < j0 + NU)
            def _():
                hid_send(k - j0).start()

            rs_first(v, NU)
            pass_m(l, a_steps(l) + k)
            pass_y(l, v - LT)

            parts((GU_IN_A[l], GU_IN_B[l]), k, functools.partial(z_gate_up_part, l))
            if l + 1 < n_layers:
                @pl.when(k == min(table(O_IN_B[l].replace("0", "-"))))
                def _():
                    w_send(l + 1).wait()

                parts((QKV_IN_B[l],), k, functools.partial(z_qkv_part, l + 1))
                parts((O_IN_B[l],), k, functools.partial(z_o_part, l + 1))

            return carry

        lax.fori_loop(0, b_steps(l), step, 0)

    for l in range(n_layers):
        pl.run_scoped(
            functools.partial(loop_a, l),
            pltpu.VMEM((W, QW + 2 * HD), BF16), pltpu.VMEM((W, QW + 2 * HD), BF16),
            pltpu.VMEM((2, QW, V) if PAIRED[l] else (1, QW, W), BF16),
            pltpu.VMEM((2, QW, V) if PAIRED[l] else (1, QW, W), BF16), pltpu.VMEM((NB, R, QW), BF16))
        pl.run_scoped(
            functools.partial(loop_b, l),
            pltpu.VMEM((HB, W), BF16), pltpu.VMEM((HB, W), BF16),
            pltpu.VMEM((HB, W), BF16), pltpu.VMEM((HB, W), BF16), pltpu.VMEM((2 * HB, W), BF16))

    def tail(v, carry):
        rs_steps(v, NU, finish_y)
        rs_sends(v, NU)
        pass_y(n_layers - 1, v - LT)
        return carry

    lax.fori_loop(NU, NU + LT + 2, tail, 0)
    for b in range(NB):
        out_send(b).wait()
        y_store(b).start()
    for b in range(NB):
        y_store(b).wait()


def solution(mesh):
    act_spec = P("fsdp", "model", None)
    col_spec = P(None, "fsdp", "model")
    row_spec = P(None, "model", "fsdp")

    def device_step(x_in, gain_attn, gain_mlp, rope_cos, rope_sin, w_q, w_k, w_v, w_o, w_gate, w_up, w_down):
        L, NB, T, D = w_q.shape[0], *x_in.shape
        W, V = D // PAIR, D // CHIPS
        HB = w_gate.shape[-1] // PAIR
        NU, R = PAIR * NB, CHIPS * CORES * T
        HD = PAIR * rope_cos.shape[-1]
        QW = w_o.shape[1]
        hbm = pl.BlockSpec(memory_space=pl.ANY)
        vmem = pl.BlockSpec(memory_space=pltpu.VMEM)
        sds = jax.ShapeDtypeStruct

        def buf(dtype, *shape):
            return pltpu.VMEM(shape, dtype)

        def sems(*shape):
            return pltpu.SemaphoreType.DMA(shape)

        args = (x_in, gain_attn, gain_mlp, rope_cos.T, rope_sin.T, w_q, w_k, w_v, w_o,
                jnp.swapaxes(w_gate, 1, -1), jnp.swapaxes(w_up, 1, -1), w_down)
        half_rows, plane_rows = (L, HB, W), (CORES, CHIPS, T, D)
        shapes = [x_in.shape, w_q.shape, w_k.shape, w_v.shape, w_o.shape[1:], half_rows, half_rows,
                  (L, NB) + plane_rows, (L, NU) + plane_rows, (L, QW, V), (L, PAIR, QW, V)]
        unit, hop = (PAIR, PAIR, T, W), (PAIR, T, V)
        in_flight, hidden, tables = LH + 1, (HB, R), (CORES, CHIPS, T, HD)
        outs = pl.pallas_call(
            _kernel,
            name="two_layers",
            in_specs=[vmem if a.ndim <= PAIR else hbm for a in args],
            out_specs=[hbm] * len(shapes),
            out_shape=[sds(shape, BF16) for shape in shapes],
            scratch_shapes=[
                buf(BF16, NB, T, D), buf(BF16, NB, T, D), buf(BF16, PAIR, T, D), buf(BF16, PAIR, *plane_rows),
                buf(F32, SLOTS, *unit), buf(F32, PAIR, *unit), buf(F32, PAIR, *unit),
                buf(F32, in_flight, *hop), buf(F32, in_flight, *hop), buf(F32, SLOTS, *hop), buf(F32, SLOTS, *hop),
                buf(F32, SLOTS, T, V), buf(F32, SLOTS, T, V), buf(BF16, in_flight, *hidden), buf(BF16, SLOTS, *hidden),
                buf(F32, *tables), buf(F32, *tables), buf(F32, CHIPS, CORES, T, HD),
                buf(BF16, NB - 1, R, QW), buf(BF16, NB, T, W), buf(BF16, in_flight, T, V)]
            + [sems(int(ch)) for ch in SEMS] + [sems(NB, CHIPS + 1), sems(NB, CHIPS + 1), sems(NU, CHIPS + 1),
                                                sems(NU, CHIPS + 1), sems(NB, PAIR), sems(NB, PAIR),
                                                sems(L, PAIR + 1), sems(L, PAIR + 1)],
            compiler_params=pltpu.CompilerParams(
                collective_id=0, has_side_effects=True, vmem_limit_bytes=67_000_000),
        )(*args)
        return outs[0]

    return jax.shard_map(
        device_step, mesh=mesh,
        in_specs=(act_spec, P(), P(), P(), P(), col_spec, col_spec, col_spec, row_spec, col_spec, col_spec, row_spec),
        out_specs=act_spec, check_vma=False)
```

```python
import functools

import jax
import jax.numpy as jnp
from jax import lax
from jax.experimental import pallas as pl
from jax.experimental.pallas import tpu as pltpu
from jax.sharding import PartitionSpec as P

EPS = 1e-5
MESH = pl.DeviceIdType.MESH
NN = (((1,), (0,)), ((), ()))
NT = (((1,), (1,)), ((), ()))
TN = (((0,), (0,)), ((), ()))
LD = 1
LX = 2
LT = LD + 2 * LX
LH = 2
LM = (7, 4)
LAGS_M = ((10, 13, 10, 12), (6, 10, 7, 14))
LAGS_Y = (4, 7)
FREE = 6
EXTRA = (7, 0)
PAIRED = (False, True)
GAP = (12, 8)
SLOTS, CHIPS, CORES, PAIR = 4, 4, 2, 2
ALIGN, LANES = 16, 128
SEMS = "4422224444444488884444" + "22888"
GU, ATTN = 18, 8

CUT_A = (29, 34)
CUT_B = (20, 19)
CUTS = 40

ATTEND = ("01234567--------", "0123-4-5--6---7---------------")
OWN = ("01234567--------", "---01234--5--6--7-------------")
OTHER = ("--------01234567", "---------0--1--2----3---456--7")
GU_IN_A = ("2000212321221211", "210002120011200220002023221010")
GU_IN_B = ("0132101231", "232")
QKV_IN_B = ("0000000000010100000001000100012010000", "")
O_IN_A = ("", "000011")
O_IN_B = ("0000000000000000000000100000110000201", "")
F32 = jnp.float32
BF16 = jnp.bfloat16


def _norm(rows, gain):
    rows = rows.astype(F32)
    mean_sq = jnp.mean(rows * rows, axis=-1, keepdims=True)
    return (rows * lax.rsqrt(mean_sq + EPS) * gain).astype(BF16)


def _kernel(
    x_ref, ga_ref, gm_ref, cos_ref, sin_ref, wq_ref, wk_ref, wv_ref, wo_ref, wg_ref, wu_ref, wd_ref,
    y_ref, rq, rk, rv, ro, rg, ru, ha, hb, rw, row,
    xbuf, mpeer, hst, hv, pown, psib, rd, t1, t2, rx, ry, rx2, ry2, hown, hrecv, cbuf, sbuf, tmp, ox, xres, mst,
    zs, zr, gs, gr, ds, dr, xs, xr, ys, yr, x2s, x2r, y2s, y2r, ms, mr, os_, or_, hs, hr, mxs, mxr,
    loc, hvs, wl, oxs, oxr, sa, ra, sb, rb, xrs, xrr, wxs, wxr,
):
    n_layers = wq_ref.shape[0]
    NB, T, D = x_ref.shape
    W, V = D // PAIR, D // CHIPS
    QW = wq_ref.shape[2]
    HD = wk_ref.shape[2]
    HB = wg_ref.shape[1] // PAIR
    R = CHIPS * CORES * T
    NU = PAIR * NB

    z = lax.axis_index("fsdp")
    m = lax.axis_index("model")
    y, x, c, q = m // 4, (m // 2) % 2, m % 2, m // 2
    qx, qy, qd = q + 1 - 2 * x, q + 2 - 4 * y, 3 - q
    zp, xp, yp, sp = (1 - z, m), (z, m + 2 - 4 * x), (z, m + 4 - 8 * y), (z, m + 1 - 2 * c)

    def lanes(start, size):
        return pl.ds(pl.multiple_of(start, LANES), size)

    def rows(start, size):
        return pl.ds(pl.multiple_of(start, ALIGN), size)

    mine, other = lanes(z * W, W), lanes((1 - z) * W, W)
    low_v, high_v = pl.ds(0, V), pl.ds(V, V)

    def even(i):
        return i % PAIR == 0

    def half_of(i):
        return i // PAIR

    def when(*conds):
        return pl.when(functools.reduce(jnp.logical_and, conds))

    def within(k, n):
        return jnp.logical_and(k >= 0, k < n)

    def lookup(table, k):
        runs = []
        for i in sorted(table):
            if runs:
                run = runs[-1]
                stride = i - run[-1]
                if table[i] == table[run[-1]] + 1 and stride in (1, PAIR) and (
                        len(run) == 1 or stride == run[-1] - run[-2]):
                    run.append(i)
                    continue
            runs.append([i])
        value, there = None, None
        for run in reversed(runs):
            first, last = run[0], run[-1]
            stride = run[1] - first if len(run) > 1 else 1
            ok = jnp.logical_and(k >= first, k <= last)
            if stride > 1:
                ok = jnp.logical_and(ok, (k - first) % stride == 0)
            val = (k - first) // stride + table[first]
            value = val if value is None else jnp.where(k <= last, val, value)
            there = ok if there is None else jnp.logical_or(there, ok)
        return value, there

    def table(text):
        return {i: int(ch) for i, ch in enumerate(text) if ch.isdigit()}

    def parts(texts, k, start):
        done = sum(int(ch) for text in texts[:-1] for ch in text)
        for i, ch in enumerate(texts[-1]):
            n = int(ch)
            if n:
                @pl.when(k == i)
                def _():
                    for j in range(done, done + n):
                        start(j)
            done += n

    barrier = pltpu.get_barrier_semaphore()
    for dev in (zp, xp, yp, sp):
        pl.semaphore_signal(barrier, inc=1, device_id=dev, device_id_type=MESH)
    pl.semaphore_wait(barrier, 4)

    def send(src, dst, s, r, dev):
        return pltpu.make_async_remote_copy(
            src_ref=src, dst_ref=dst, send_sem=s, recv_sem=r, device_id=dev, device_id_type=MESH)

    def z_q(l):
        return send(wq_ref.at[l], rq.at[l], zs.at[0], zr.at[0], zp)

    def z_k(l):
        return send(wk_ref.at[l], rk.at[l], zs.at[1], zr.at[1], zp)

    def z_v(l):
        return send(wv_ref.at[l], rv.at[l], zs.at[2], zr.at[2], zp)

    def z_o(l):
        return send(wo_ref.at[l], ro, zs.at[3], zr.at[3], zp)

    mine_h, theirs_h = rows(z * HB, HB), rows((1 - z) * HB, HB)

    def z_g(l):
        return send(wg_ref.at[l, theirs_h], rg.at[l], gs.at[0], gr.at[0], zp)

    def z_u(l):
        return send(wu_ref.at[l, theirs_h], ru.at[l], gs.at[1], gr.at[1], zp)

    def z_gate_up_part(l, j):
        size = HB // GU
        ref, out, i = (wg_ref, rg, 0) if j < GU else (wu_ref, ru, 1)
        at = (j % GU) * size
        send(ref.at[l, rows((1 - z) * HB + at, size)], out.at[l, pl.ds(at, size)], gs.at[i], gr.at[i], zp).start()

    def z_qkv_part(l, j):
        size = W // ATTN
        at = pl.ds(j * size, size)
        for i, (ref, out) in enumerate(((wq_ref, rq), (wk_ref, rk), (wv_ref, rv))):
            send(ref.at[l, at], out.at[l, at], zs.at[i], zr.at[i], zp).start()

    def z_o_part(l, j):
        size = QW // ATTN
        for d in z_oq(l, pl.ds(j * size, size)):
            d.start()

    def cut_of(share):
        return max(1, D // LANES * share // CUTS) * LANES

    def cut_a(l):
        return cut_of(CUT_A[l])

    def cut_b(l):
        return cut_of(CUT_B[l])

    def ag_own(h, s, r, u):
        own = h.at[u, 0, q]
        return [send(own, own, s.at[u], r.at[u, i], dev) for i, dev in enumerate((xp, yp))]

    def ag_fwd(h, s, r, u, cut):
        from_x, from_y = h.at[u, 0, qx, :, pl.ds(0, cut)], h.at[u, 0, qy, :, pl.ds(cut, D - cut)]
        return [send(from_x, from_x, s.at[u], r.at[u, PAIR], yp), send(from_y, from_y, s.at[u], r.at[u, PAIR], xp)]

    def ag_sib(h, s, r, u):
        return send(h.at[u, 0], h.at[u, 1], s.at[u], r.at[u, CHIPS - 1], sp)

    def ag_send_own(h, s, r, u):
        for d in ag_own(h, s, r, u):
            d.start()

    def ag_fwd1(h, s, r, u, cut):
        for own, fwd in zip(ag_own(h, s, r, u), ag_fwd(h, s, r, u, cut)):
            own.wait_recv()
            fwd.start()

    def ag_fwd2(h, s, r, u, cut):
        block = h.at[u, 0, qd]
        send(block, block, s.at[u], r.at[u, PAIR], xp).wait_recv()
        ag_sib(h, s, r, u).start()

    def ag_local(h, u):
        return pltpu.make_async_copy(h.at[u], hv.at[u % PAIR], hvs.at[u % PAIR])

    def ag_load(h, s, r, u):
        ag_sib(h, s, r, u).wait_recv()
        ag_local(h, u).start()

    def ag_finish(h, s, r, u, cut):
        ag_local(h, u).wait()
        seven = ha.at[0, pl.ds(0, NB - 1), 0, 0]
        send(seven, seven, s.at[u], r.at[u, 0], sp).wait_send()

    def y_store(b):
        return pltpu.make_async_copy(xbuf.at[b], y_ref.at[b], oxs.at[b])

    def h_store(h, u, j):
        return pltpu.make_async_copy(hst.at[j], h.at[u, 0, q], loc.at[j])

    def rs_d(u):
        return send(psib.at[u % PAIR], rd.at[u % PAIR], ds.at[u % PAIR], dr.at[u % PAIR], sp)

    def rs_x(u):
        i = u % SLOTS
        return send(pown.at[i, :, 1 - x, :, low_v], rx.at[i], xs.at[i], xr.at[i], xp)

    def rs_y(u):
        i = u % SLOTS
        return send(pown.at[i, 1 - y, :, :, high_v], ry.at[i], ys.at[i], yr.at[i], yp)

    def ra_d(u):
        return send(psib.at[u % PAIR, :, :, :, low_v], rd.at[u % PAIR, :, :, :, low_v],
                    ds.at[u % PAIR], dr.at[u % PAIR], sp)

    def ra_y(u):
        i = u % SLOTS
        return send(pown.at[i, 1 - y, :, :, low_v], ry.at[i], ys.at[i], yr.at[i], yp)

    def ra_m(u, b, half):
        cols = lanes(half * W + x * V, V)
        return send(mst.at[u % (LH + 1)], xbuf.at[b, :, cols], mxs.at[u % SLOTS], mxr.at[u % SLOTS], xp)

    def o_send(o_all, b):
        return send(o_all.at[b], ox.at[b % (NB - 1)], oxs.at[b], oxr.at[b], xp)

    def res_send(b, half):
        src = lanes(half * W + (1 - x) * V, V)
        dst = lanes(half * V, V)
        return send(xbuf.at[b, :, src], xres.at[b, :, dst], xrs.at[b, half], xrr.at[b, half], xp)

    def w_send(l):
        cols = lanes((1 - x) * V, V)
        return send(wo_ref.at[l, :, cols], rw.at[l], wxs.at[l, 0], wxr.at[l, 0], xp)

    def z_oq(l, rows=slice(None)):
        cols = lanes(x * V, V)
        return (send(wo_ref.at[l, rows, cols], row.at[l, 0, rows], wxs.at[l, 1], wxr.at[l, 1], zp),
                send(rw.at[l, rows], row.at[l, 1, rows], wxs.at[l, 2], wxr.at[l, 2], zp))

    def rs_x2(u):
        i = u % SLOTS
        return send(t2.at[u % (LH + 1), 1 - x], rx2.at[i], x2s.at[i], x2r.at[i], xp)

    def rs_y2(u):
        i = u % SLOTS
        return send(t1.at[u % (LH + 1), 1 - y], ry2.at[i], y2s.at[i], y2r.at[i], yp)

    def store_product(u, pairs, width):
        half = W // 2
        for j in range(width // half):
            cols = pl.ds(j * half, half)
            acc = None
            for a, w, rows in pairs:
                wv_ = w[:, cols] if rows is None else w[rows, cols]
                p = lax.dot_general(a, wv_, TN if rows is not None else NN, preferred_element_type=F32)
                acc = p if acc is None else acc + p
            pown[u % SLOTS, :, :, :, cols] = acc[: R // 2].reshape(2, 2, T, half)
            psib[u % PAIR, :, :, :, cols] = acc[R // 2:].reshape(2, 2, T, half)

    def rs_stage2(u):
        rs_d(u).wait()
        pown[u % SLOTS] = pown[u % SLOTS] + rd[u % PAIR]

    def rs_stage3(u):
        i = u % SLOTS
        rs_x(u).wait()
        rs_y(u).wait()
        t1[u % (LH + 1)] = pown[i, :, x, :, low_v] + rx[i]
        t2[u % (LH + 1)] = pown[i, y, :, :, high_v] + ry[i]

    def rs_stage4(u):
        i = u % SLOTS
        rs_x2(u).wait()
        rs_y2(u).wait()
        return t1[u % (LH + 1), y] + ry2[i], t2[u % (LH + 1), x] + rx2[i]

    def rs_steps(k, n, finish):
        @pl.when(jnp.logical_and(k >= LD, k < n + LD))
        def _():
            rs_stage2(k - LD)

        @pl.when(jnp.logical_and(k >= LD + LX, k < n + LD + LX))
        def _():
            rs_stage3(k - LD - LX)

        @pl.when(jnp.logical_and(k >= LT, k < n + LT))
        def _():
            finish(k - LT, *rs_stage4(k - LT))

    def rs_first(k, n):
        pl.when(within(k, n))(lambda: rs_d(k).start())

    def rs_sends(k, n):
        @pl.when(jnp.logical_and(k >= LD, k < n + LD))
        def _():
            rs_x(k - LD).start()
            rs_y(k - LD).start()

        @pl.when(jnp.logical_and(k >= LD + LX, k < n + LD + LX))
        def _():
            rs_x2(k - LD - LX).start()
            rs_y2(k - LD - LX).start()

    def m_send(b):
        return send(xbuf.at[b], mpeer.at[b], ms.at[b], mr.at[b], zp)

    def out_send(b):
        return send(mpeer.at[b, :, mine], xbuf.at[b, :, mine], os_.at[b], or_.at[b], zp)

    def hid_send(u):
        i = u % SLOTS
        return send(hown.at[u % (LH + 1)], hrecv.at[i], hs.at[i], hr.at[i], zp)

    for d in (z_q(0), z_k(0), z_v(0), z_oq(0)[0] if PAIRED[0] else z_o(0)):
        d.start()
    first = [pltpu.make_async_copy(x_ref, xbuf, wl.at[0])]
    for d in first:
        d.start()
    for d in first:
        d.wait()

    def first_rows(b, carry):
        hst[0] = _norm(xbuf[b], ga_ref[pl.ds(0, 1), :])
        d = h_store(ha.at[0], b, 0)
        d.start()
        d.wait()
        ag_send_own(ha.at[0], sa, ra, b)
        return carry

    lax.fori_loop(0, NB, first_rows, 0)
    if PAIRED[0]:
        w_send(0).start()
        for b in range(NB):
            for half in range(PAIR):
                res_send(b, half).start()

    def first_forward(i, carry):
        ag_fwd1(ha.at[0], sa, ra, i, cut_a(0))

        @pl.when(i >= 1)
        def _():
            ag_fwd2(ha.at[0], sa, ra, i - 1, cut_a(0))

        return carry

    for ref, buf, sign in ((cos_ref, cbuf, 1.0), (sin_ref, sbuf, -1.0)):
        tab = ref[...].T
        tmp[...] = jnp.concatenate([sign * tab, tab], axis=1).reshape(4, 2, T, HD)
        buf[0] = tmp[:, c]
        buf[1] = tmp[:, 1 - c]

    lax.fori_loop(0, NB, first_forward, 0)
    w_send(1).start()
    def pass_m(l, k):
        h = hb.at[l]
        cut = cut_b(l)
        wait_m = LM[l]

        def at(lag, run):
            b, ok = lookup(table(OTHER[l]), k - lag - LT)
            pl.when(ok)(lambda: run(b))

        def own(b):
            return PAIR * b + z

        def theirs(b):
            return PAIR * b + 1 - z

        def send_own(b):
            h_store(h, own(b), 0).wait()
            ag_send_own(h, sb, rb, own(b))

        def start_own(b):
            hst[0] = _norm(xbuf[b], gm_ref[pl.ds(l, 1), :])
            h_store(h, own(b), 0).start()
            m_send(b).start()

        def send_theirs(b):
            h_store(h, theirs(b), 1).wait()
            ag_send_own(h, sb, rb, theirs(b))

        def start_theirs(b):
            m_send(b).wait()
            hst[1] = _norm(mpeer[b], gm_ref[pl.ds(l, 1), :])
            h_store(h, theirs(b), 1).start()

        own_1, own_2, theirs_1, theirs_2 = LAGS_M[l]
        at(1, send_own)
        at(0, start_own)
        at(wait_m + 1, send_theirs)
        at(wait_m, start_theirs)
        at(own_1, lambda b: ag_fwd1(h, sb, rb, own(b), cut))
        at(theirs_1, lambda b: ag_fwd1(h, sb, rb, theirs(b), cut))
        at(own_2, lambda b: ag_fwd2(h, sb, rb, own(b), cut))
        at(theirs_2, lambda b: ag_fwd2(h, sb, rb, theirs(b), cut))

    def pass_y(l, s):
        last = l + 1 == n_layers
        free = FREE if last else 0

        @when(s >= free, s < NU, s % PAIR == 1 - z)
        def _():
            out_send(half_of(s)).start()

        if last:
            @pl.when(s == free)
            def _():
                for b in range(half_of(free)):
                    out_send(b).start()

        def at(lag, run):
            i = s - lag - 1
            when(within(i, NU), even(i))(lambda: run(half_of(i)))

        def got(b):
            out_send(b).wait()
            hst[0] = _norm(xbuf[b], ga_ref[pl.ds(l + 1, 1), :])
            h_store(ha.at[l + 1], b, 0).start()
            for half in range(PAIR):
                res_send(b, half).start()

        if not last:
            at(1, got)
            h, cut = ha.at[l + 1], cut_a(l + 1)

            def send_own(b):
                h_store(h, b, 0).wait()
                ag_send_own(h, sa, ra, b)

            at(2, send_own)
            at(LAGS_Y[0], lambda b: ag_fwd1(h, sa, ra, b, cut))
            at(LAGS_Y[1], lambda b: ag_fwd2(h, sa, ra, b, cut))

    def add(buf, b, start, low, high):
        for at, part in ((start, low), (start + V, high)):
            cols = lanes(at, V)
            buf[b, :, cols] = (buf[b, :, cols].astype(F32) + part).astype(BF16)

    def finish_y(s, low, high):
        b = half_of(s)
        pl.when(s % PAIR == z)(lambda: add(xbuf, b, z * W, low, high))
        pl.when(s % PAIR == 1 - z)(lambda: add(mpeer, b, z * W, low, high))

    def finish_m(u, low, high):
        half = z + (u // NB) * (1 - z - z)
        add(xbuf, u % NB, half * W, low, high)

    def a_steps(l):
        return len(ATTEND[l])

    def a_attend(l, k):
        return lookup(table(ATTEND[l]), k)

    def a_unit(l, k):
        own, oth = table(OWN[l]), table(OTHER[l])
        b_own, is_own = lookup(own, k)
        b_oth, is_oth = lookup(oth, k)
        u, _ = lookup({i: n for n, i in enumerate(sorted({**own, **oth}))}, k)
        return jnp.where(is_own, b_own, b_oth), u, is_own, is_oth

    def a_stages(l, k):
        if not PAIRED[l]:
            rs_steps(k, NU, finish_m)
            return

        def at(lag):
            b, u, own, oth = a_unit(l, k - lag)
            half = jnp.where(own, z, 1 - z)
            return b, u, half, jnp.logical_or(own, oth)

        _, u2, _, ok2 = at(LD)

        @pl.when(ok2)
        def _():
            ra_d(u2).wait()
            cols = low_v
            pown[u2 % SLOTS, :, :, :, cols] = pown[u2 % SLOTS, :, :, :, cols] + rd[u2 % PAIR, :, :, :, cols]

        b3, u3, half3, ok3 = at(LD + LX)

        @pl.when(ok3)
        def _():
            i = u3 % SLOTS
            ra_y(u3).wait()
            res_send(b3, half3).wait_recv()
            cols = lanes(half3 * W + x * V, V)
            xbuf[b3, :, cols] = (xbuf[b3, :, cols].astype(F32)
                                 + (pown[i, y, x, :, low_v] + ry[i, x])).astype(BF16)
            res = xres[b3, :, lanes(half3 * V, V)].astype(F32)
            mst[u3 % (LH + 1)] = (res + (pown[i, y, 1 - x, :, low_v] + ry[i, 1 - x])).astype(BF16)

        b4, u4, half4, ok4 = at(LT)
        pl.when(ok4)(lambda: ra_m(u4, b4, half4).wait())

    def a_first(l, k):
        _, u, own, oth = a_unit(l, k)
        first = ra_d if PAIRED[l] else rs_d
        pl.when(jnp.logical_or(own, oth))(lambda: first(u).start())

    def a_sends(l, k):
        if not PAIRED[l]:
            rs_sends(k, NU)
            return

        def at(lag):
            b, u, own, oth = a_unit(l, k - lag)
            return b, u, jnp.where(own, z, 1 - z), jnp.logical_or(own, oth)

        _, u2, _, ok2 = at(LD)
        pl.when(ok2)(lambda: ra_y(u2).start())
        b3, u3, half3, ok3 = at(LD + LX)
        pl.when(ok3)(lambda: ra_m(u3, b3, half3).start())

    def b_steps(l):
        return GAP[l] + LH + NU + EXTRA[l]

    def pos_of(r):
        rail = r // (CHIPS * T)
        return CORES * T * ((r // T) % CHIPS) + T * ((c + rail) % CORES) + r % T

    def attend(l, b, h, wa_o, wa_r, o_all):
        ag_finish(h, sa, ra, b, cut_a(l))
        i = b % PAIR
        acc = jnp.dot(hv[i, :, :, :, mine].reshape(R, W), wa_o[...], preferred_element_type=F32)
        acc += jnp.dot(hv[i, :, :, :, other].reshape(R, W), wa_r[...], preferred_element_type=F32)
        qkv = acc.astype(BF16)
        cosv = cbuf[...].reshape(R, HD)
        sinv = sbuf[...].reshape(R, HD)

        def rope(t):
            t = t.astype(F32)
            return (t * cosv + pltpu.roll(t, HD // 2, 1) * sinv).astype(BF16)

        mask = pos_of(lax.broadcasted_iota(jnp.int32, (R, R), 0)) >= pos_of(
            lax.broadcasted_iota(jnp.int32, (R, R), 1))
        kk = rope(qkv[:, QW:QW + HD])
        vv = qkv[:, QW + HD:]
        for g in range(QW // HD):
            sc = lax.dot_general(rope(qkv[:, g * HD:(g + 1) * HD]), kk, NT, preferred_element_type=F32)
            sc = jnp.where(mask, sc * HD ** -0.5, -jnp.inf)
            e = jnp.exp(sc - jnp.max(sc, axis=-1, keepdims=True))
            p = (e / jnp.sum(e, axis=-1, keepdims=True)).astype(BF16)
            o_all[b, :, g * HD:(g + 1) * HD] = jnp.dot(p, vv, preferred_element_type=F32).astype(BF16)

    def loop_a(l, wa_o, wa_r, w_own, w_oth, o_all):
        h = ha.at[l]
        my_v = lanes(x * V, V)
        loads = [pltpu.make_async_copy(wq_ref.at[l], wa_o.at[:, pl.ds(0, QW)], wl.at[0]),
                 pltpu.make_async_copy(wk_ref.at[l], wa_o.at[:, pl.ds(QW, HD)], wl.at[1]),
                 pltpu.make_async_copy(wv_ref.at[l], wa_o.at[:, pl.ds(QW + HD, HD)], wl.at[2]),
                 pltpu.make_async_copy(wo_ref.at[l, :, my_v] if PAIRED[l] else wo_ref.at[l],
                                       w_own.at[0], wl.at[3])]
        from_x = pltpu.make_async_copy(rw.at[l], w_own.at[1], wl.at[7]) if PAIRED[l] else None
        if l > 0:
            loads.append(from_x)
        for d in loads:
            d.start()
        ag_load(h, sa, ra, 0)
        for d in (z_q(l), z_k(l), z_v(l)):
            d.wait()
        more = [pltpu.make_async_copy(rq.at[l], wa_r.at[:, pl.ds(0, QW)], wl.at[4]),
                pltpu.make_async_copy(rk.at[l], wa_r.at[:, pl.ds(QW, HD)], wl.at[5]),
                pltpu.make_async_copy(rv.at[l], wa_r.at[:, pl.ds(QW + HD, HD)], wl.at[6])]
        for d in more:
            d.start()
        for d in loads + more:
            d.wait()
        first_other = min(table(OTHER[l]))

        def step(k, carry):
            if l == 0:
                @pl.when(k == 0)
                def _():
                    ag_fwd2(h, sa, ra, NB - 1, cut_a(0))

            bn, next_ok = a_attend(l, k + 1)
            pl.when(next_ok)(lambda: ag_load(h, sa, ra, bn))
            ba, ok = a_attend(l, k)
            pl.when(ok)(lambda: attend(l, ba, h, wa_o, wa_r, o_all))
            if l > 0:
                rs_steps(NU + EXTRA[l - 1] + k, NU, finish_y)
            a_stages(l, k)
            if l > 0:
                rs_sends(NU + EXTRA[l - 1] + k, NU)
            if PAIRED[l]:
                @pl.when(ok)
                def _():
                    for half in range(2):
                        res_send(ba, half).wait_send()
                    o_send(o_all, ba).start()

            a_sends(l, k)
            b, u, own, oth = a_unit(l, k)

            if PAIRED[l] and l == 0:
                @pl.when(k == min(table(OWN[l])))
                def _():
                    w_send(l).wait()
                    z_oq(l)[1].start()
                    from_x.start()
                    from_x.wait()

            @pl.when(own)
            def _():
                if not PAIRED[l]:
                    store_product(u, [(o_all[b], w_own.at[0], None)], W)
                else:
                    o_send(o_all, b).wait()
                    store_product(u, [(o_all[b], w_own.at[0], None), (ox[b % (NB - 1)], w_own.at[1], None)], V)

            @pl.when(k == first_other)
            def _():
                got = z_oq(l) if PAIRED[l] else (z_o(l),)
                for d in got:
                    d.wait()
                if not PAIRED[l]:
                    into = [pltpu.make_async_copy(ro, w_oth.at[0], wl.at[5])]
                else:
                    into = [pltpu.make_async_copy(row.at[l, i], w_oth.at[i], wl.at[5 + i]) for i in range(2)]
                for d in into:
                    d.start()
                for d in into:
                    d.wait()

            @pl.when(oth)
            def _():
                if not PAIRED[l]:
                    store_product(u, [(o_all[b], w_oth.at[0], None)], W)
                else:
                    store_product(u, [(o_all[b], w_oth.at[0], None), (ox[b % (NB - 1)], w_oth.at[1], None)], V)

            a_first(l, k)
            if l > 0:
                pass_y(l - 1, NU + EXTRA[l - 1] + k - LT)
            pass_m(l, k)

            parts((O_IN_B[l - 1], O_IN_A[l]), k, functools.partial(z_o_part, l))
            parts((GU_IN_A[l],), k, functools.partial(z_gate_up_part, l))
            return carry

        lax.fori_loop(0, a_steps(l), step, 0)

    def loop_b(l, g_o, g_r, u_o, u_r, wd_v):
        h = hb.at[l]
        j0 = GAP[l]
        loads = [pltpu.make_async_copy(wg_ref.at[l, mine_h], g_o, wl.at[0]),
                 pltpu.make_async_copy(wu_ref.at[l, mine_h], u_o, wl.at[1]),
                 pltpu.make_async_copy(wd_ref.at[l], wd_v, wl.at[2])]
        more = [pltpu.make_async_copy(rg.at[l], g_r, wl.at[3]),
                pltpu.make_async_copy(ru.at[l], u_r, wl.at[4])]
        for d in loads:
            d.start()

        def step(k, carry):
            @pl.when(k == j0 - 1)
            def _():
                z_g(l).wait()
                more[0].start()
                for d in loads:
                    d.wait()
                more[0].wait()

            @pl.when(k == j0)
            def _():
                z_u(l).wait()
                more[1].start()
                more[1].wait()

            @when(k >= j0 - 1, k < j0 + NU - 1)
            def _():
                ag_load(h, sb, rb, k - j0 + 1)

            @when(k >= j0, k < j0 + NU)
            def _():
                u = k - j0
                ag_finish(h, sb, rb, u, cut_b(l))
                i = u % PAIR
                hm = hv[i, :, :, :, mine].reshape(R, W)
                ho = hv[i, :, :, :, other].reshape(R, W)
                gate = lax.dot_general(g_o[...], hm, NT, preferred_element_type=F32)
                gate += lax.dot_general(g_r[...], ho, NT, preferred_element_type=F32)
                up = lax.dot_general(u_o[...], hm, NT, preferred_element_type=F32)
                up += lax.dot_general(u_r[...], ho, NT, preferred_element_type=F32)
                hown[u % (LH + 1)] = (jax.nn.silu(gate) * up).astype(BF16)

            v = k - j0 - LH
            a_stages(l, a_steps(l) + k)
            rs_steps(v, NU, finish_y)

            a_sends(l, a_steps(l) + k)
            rs_sends(v, NU)

            @pl.when(within(v, NU))
            def _():
                hid_send(v).wait()
                store_product(v, [(hown[v % (LH + 1)], wd_v, mine_h), (hrecv[v % SLOTS], wd_v, theirs_h)], W)

            @when(k >= j0, k < j0 + NU)
            def _():
                hid_send(k - j0).start()

            rs_first(v, NU)
            pass_m(l, a_steps(l) + k)
            pass_y(l, v - LT)

            parts((GU_IN_A[l], GU_IN_B[l]), k, functools.partial(z_gate_up_part, l))
            if l + 1 < n_layers:
                @pl.when(k == min(table(O_IN_B[l].replace("0", "-"))))
                def _():
                    w_send(l + 1).wait()

                parts((QKV_IN_B[l],), k, functools.partial(z_qkv_part, l + 1))
                parts((O_IN_B[l],), k, functools.partial(z_o_part, l + 1))

            return carry

        lax.fori_loop(0, b_steps(l), step, 0)

    for l in range(n_layers):
        pl.run_scoped(
            functools.partial(loop_a, l),
            pltpu.VMEM((W, QW + 2 * HD), BF16), pltpu.VMEM((W, QW + 2 * HD), BF16),
            pltpu.VMEM((2, QW, V) if PAIRED[l] else (1, QW, W), BF16),
            pltpu.VMEM((2, QW, V) if PAIRED[l] else (1, QW, W), BF16), pltpu.VMEM((NB, R, QW), BF16))
        pl.run_scoped(
            functools.partial(loop_b, l),
            pltpu.VMEM((HB, W), BF16), pltpu.VMEM((HB, W), BF16),
            pltpu.VMEM((HB, W), BF16), pltpu.VMEM((HB, W), BF16), pltpu.VMEM((2 * HB, W), BF16))

    def tail(v, carry):
        rs_steps(v, NU, finish_y)
        rs_sends(v, NU)
        pass_y(n_layers - 1, v - LT)
        return carry

    lax.fori_loop(NU, NU + LT + 2, tail, 0)
    for b in range(NB):
        out_send(b).wait()
        y_store(b).start()
    for b in range(NB):
        y_store(b).wait()


def solution(mesh):
    act_spec = P("fsdp", "model", None)
    col_spec = P(None, "fsdp", "model")
    row_spec = P(None, "model", "fsdp")

    def device_step(x_in, gain_attn, gain_mlp, rope_cos, rope_sin, w_q, w_k, w_v, w_o, w_gate, w_up, w_down):
        L, NB, T, D = w_q.shape[0], *x_in.shape
        W, V = D // PAIR, D // CHIPS
        HB = w_gate.shape[-1] // PAIR
        NU, R = PAIR * NB, CHIPS * CORES * T
        HD = PAIR * rope_cos.shape[-1]
        QW = w_o.shape[1]
        hbm = pl.BlockSpec(memory_space=pl.ANY)
        vmem = pl.BlockSpec(memory_space=pltpu.VMEM)
        sds = jax.ShapeDtypeStruct

        def buf(dtype, *shape):
            return pltpu.VMEM(shape, dtype)

        def sems(*shape):
            return pltpu.SemaphoreType.DMA(shape)

        args = (x_in, gain_attn, gain_mlp, rope_cos.T, rope_sin.T, w_q, w_k, w_v, w_o,
                jnp.swapaxes(w_gate, 1, -1), jnp.swapaxes(w_up, 1, -1), w_down)
        half_rows, plane_rows = (L, HB, W), (CORES, CHIPS, T, D)
        shapes = [x_in.shape, w_q.shape, w_k.shape, w_v.shape, w_o.shape[1:], half_rows, half_rows,
                  (L, NB) + plane_rows, (L, NU) + plane_rows, (L, QW, V), (L, PAIR, QW, V)]
        unit, hop = (PAIR, PAIR, T, W), (PAIR, T, V)
        in_flight, hidden, tables = LH + 1, (HB, R), (CORES, CHIPS, T, HD)
        outs = pl.pallas_call(
            _kernel,
            name="two_layers",
            in_specs=[vmem if a.ndim <= PAIR else hbm for a in args],
            out_specs=[hbm] * len(shapes),
            out_shape=[sds(shape, BF16) for shape in shapes],
            scratch_shapes=[
                buf(BF16, NB, T, D), buf(BF16, NB, T, D), buf(BF16, PAIR, T, D), buf(BF16, PAIR, *plane_rows),
                buf(F32, SLOTS, *unit), buf(F32, PAIR, *unit), buf(F32, PAIR, *unit),
                buf(F32, in_flight, *hop), buf(F32, in_flight, *hop), buf(F32, SLOTS, *hop), buf(F32, SLOTS, *hop),
                buf(F32, SLOTS, T, V), buf(F32, SLOTS, T, V), buf(BF16, in_flight, *hidden), buf(BF16, SLOTS, *hidden),
                buf(F32, *tables), buf(F32, *tables), buf(F32, CHIPS, CORES, T, HD),
                buf(BF16, NB - 1, R, QW), buf(BF16, NB, T, W), buf(BF16, in_flight, T, V)]
            + [sems(int(ch)) for ch in SEMS] + [sems(NB), sems(NB, CHIPS), sems(NU), sems(NU, CHIPS),
                                                sems(NB, PAIR), sems(NB, PAIR),
                                                sems(L, PAIR + 1), sems(L, PAIR + 1)],
            compiler_params=pltpu.CompilerParams(
                collective_id=0, has_side_effects=True, vmem_limit_bytes=67_000_000),
        )(*args)
        return outs[0]

    return jax.shard_map(
        device_step, mesh=mesh,
        in_specs=(act_spec, P(), P(), P(), P(), col_spec, col_spec, col_spec, row_spec, col_spec, col_spec, row_spec),
        out_specs=act_spec, check_vma=False)
```
